32 devices in a mesh: gx: 8 (over y, x, core), gy: 4 (over z).
Axes of the slice: x: 2, y: 2, z: 4, core: 2. Of those that a mesh axis runs over, the one named last changes fastest.
Arguments:
- positions: float32 [3, 8, 4, 128], P(None, 'gx', 'gy'), may hold values from 0 to 384, as said below
- neighbours: int32 [32, 8, 4, 128], P(None, 'gx', 'gy'), may hold values from 0 to 1151, as said below
- live_count: int32 [8, 4], P('gx', 'gy'), may hold values from 16 to 128, as said below
- stencil_base: int32 [3, 8, 4, 128], P(None, 'gx', 'gy'), may hold values from -1 to 383, as said below
- spline_weight: float32 [3, 4, 8, 4, 128], P(None, None, 'gx', 'gy'), may hold values from 0 to 1, as said below
- spline_slope: float32 [3, 4, 8, 4, 128], P(None, None, 'gx', 'gy'), may hold values from -1 to 1, as said below
- embed_scale: float32 [100], replicated, may hold values from -12 to 12
- embed_bias: float32 [100], replicated, may hold values from -4 to 4
- desc_gain: float32 [1600], replicated, may hold values from 0.25 to 1.75
- fit_in: bfloat16 [128, 1600], replicated, may hold values from -0.15625 to 0.15625
- fit_bias: float32 [128], replicated, may hold values from -3 to 3
- fit_hidden: bfloat16 [128, 128], replicated, may hold values from -0.5 to 0.5
- fit_bias_two: float32 [128], replicated, may hold values from -3 to 3
- fit_out: float32 [128], replicated, may hold values from -0.5 to 0.5
Outputs:
- centroid_energy: float32 [8, 4, 128], P('gx', 'gy')
- centroid_force: float32 [3, 8, 4, 128], P(None, 'gx', 'gy')
The draws below stay inside these ranges and needn't reach their ends.
Inputs may be any that keep to these rules, and one draw needn't show every extreme that they name: `live_count`: slots below a column's count are live; some column has all 128 slots live. `neighbours`: every entry names a live slot of one of the nine blocks of the column's neighbourhood. `stencil_base`: along x the base lies in -1 to 46, along y in -1 to 94, along z in 0 to 383. `positions`: x lies in 0 to 48, y in 0 to 96, z in 0 to 384. `spline_weight`: cubic B-spline weights of a fraction in [0, 1) for each axis; the four weights sum to one. `spline_slope`: the derivatives of those weights with respect to the fraction.
All inputs are finite; a program needn't handle non-finite values.
Results may differ from the reference program's by a relative error of at most 0.006.
The reference program's roundings to bfloat16 on the way (of `normed`) count: a program that leaves them out, or rounds other values in their place, can miss the bound.
Values sent between devices are 32-bit elements; how exact they have to be, the bound alone decides.
A program may use at most 128 MiB of HBM per device.

```python
import math
import jax
import jax.numpy as jnp
from jax import lax

GRID = 384
EMB = 100
AXIS = 16
FIT = 128
NEIGH = 32
ATOM_DEV = 128
DESC = 1600
CX = 48
CY = 96
N_GX = 8
N_GY = 4


def live_counts(key):
    fewest = ATOM_DEV // 8
    spread_range = ATOM_DEV - fewest
    picked = jax.random.randint(jax.random.fold_in(key, 101), (N_GX, N_GY), 0, spread_range + 1)
    counts = fewest + picked * picked // spread_range
    fullest = jax.random.randint(jax.random.fold_in(key, 102), (), 0, N_GX * N_GY)
    flat = jnp.where(jnp.arange(N_GX * N_GY) == fullest, ATOM_DEV, counts.reshape(-1))
    return flat.reshape(N_GX, N_GY).astype(jnp.int32)


def draw_live_count(key, part):
    return live_counts(key)


def draw_neighbours(key, part):
    counts = live_counts(key)
    shape = (NEIGH, N_GX, N_GY, ATOM_DEV)
    block = jax.random.randint(jax.random.fold_in(key, 103), shape, 0, 9)
    stride_x = block // 3 - 1
    stride_y = block % 3 - 1
    rows = lax.broadcasted_iota(jnp.int32, shape, 1)
    cols = lax.broadcasted_iota(jnp.int32, shape, 2)
    slots = lax.broadcasted_iota(jnp.int32, shape, 3)
    other = counts[(rows + stride_x) % N_GX, (cols + stride_y) % N_GY]
    owned = counts[rows, cols]
    aligned = jnp.minimum(slots, owned - 1) * other // owned
    jitter = jax.random.randint(jax.random.fold_in(key, 104), shape, -3, 4)
    chosen = jnp.clip(aligned + jitter, 0, other - 1)
    return (block * ATOM_DEV + chosen).astype(jnp.int32)


def draw_positions(key, part):
    counts = live_counts(key)
    shape = (N_GX, N_GY, ATOM_DEV)
    fraction = jax.random.uniform(jax.random.fold_in(key, 105), (3,) + shape, jnp.float32)
    slots = lax.broadcasted_iota(jnp.int32, shape, 2)
    owned = counts[:, :, None]
    height = jnp.where(slots < owned, (slots.astype(jnp.float32) + fraction[2]) / owned.astype(jnp.float32), fraction[2])
    coord_x = fraction[0] * (GRID // N_GX)
    coord_y = fraction[1] * (GRID // N_GY)
    coord_z = jnp.minimum(height * GRID, GRID * 0.999)
    return jnp.stack([coord_x, coord_y, coord_z]).astype(jnp.float32)


def draw_stencil_base(key, part):
    shape = (N_GX, N_GY, ATOM_DEV)
    base_x = jax.random.randint(jax.random.fold_in(key, 107), shape, -1, GRID // N_GX - 1)
    base_y = jax.random.randint(jax.random.fold_in(key, 108), shape, -1, GRID // N_GY - 1)
    base_z = jax.random.randint(jax.random.fold_in(key, 109), shape, 0, GRID)
    return jnp.stack([base_x, base_y, base_z]).astype(jnp.int32)


def spline_fraction(key):
    fraction = jax.random.uniform(jax.random.fold_in(key, 106), (3, N_GX, N_GY, ATOM_DEV), jnp.float32)
    return fraction


def draw_spline_weight(key, part):
    fraction = spline_fraction(key)
    remain = 1.0 - fraction
    cube = fraction * fraction * fraction
    square = fraction * fraction
    values = [remain * remain * remain / 6.0, (3.0 * cube - 6.0 * square + 4.0) / 6.0, (-3.0 * cube + 3.0 * square + 3.0 * fraction + 1.0) / 6.0, cube / 6.0]
    return jnp.stack(values, axis=1).astype(jnp.float32)


def draw_spline_slope(key, part):
    fraction = spline_fraction(key)
    remain = 1.0 - fraction
    square = fraction * fraction
    values = [-0.5 * remain * remain, (3.0 * square - 4.0 * fraction) / 2.0, (-3.0 * square + 2.0 * fraction + 1.0) / 2.0, 0.5 * square]
    return jnp.stack(values, axis=1).astype(jnp.float32)


def normal_values(stream_key, shape, spread, limit, kind=jnp.bfloat16):
    values = jax.random.normal(stream_key, shape, jnp.float32) * spread
    return jnp.minimum(jnp.maximum(values, -limit), limit).astype(kind)


def setup_inputs(seed: int = 0) -> dict:
    keys = jax.random.split(jax.random.key(seed), 15)
    return {
        "positions": draw_positions(jax.random.fold_in(keys[14], 71), 0),
        "neighbours": draw_neighbours(jax.random.fold_in(keys[14], 71), 0),
        "live_count": draw_live_count(jax.random.fold_in(keys[14], 71), 0),
        "stencil_base": draw_stencil_base(jax.random.fold_in(keys[14], 71), 0),
        "spline_weight": draw_spline_weight(jax.random.fold_in(keys[14], 71), 0),
        "spline_slope": draw_spline_slope(jax.random.fold_in(keys[14], 71), 0),
        "embed_scale": normal_values(keys[6], (EMB,), 3.0, 12.0, jnp.float32),
        "embed_bias": normal_values(keys[7], (EMB,), 1.0, 4.0, jnp.float32),
        "desc_gain": jnp.clip(1.0 + 0.15 * jax.random.normal(keys[8], (DESC,), jnp.float32), 0.25, 1.75),
        "fit_in": normal_values(keys[9], (FIT, DESC), DESC ** -0.5, 0.15625),
        "fit_bias": normal_values(keys[10], (FIT,), 0.5, 3.0, jnp.float32),
        "fit_hidden": normal_values(keys[11], (FIT, FIT), FIT ** -0.5, 0.5),
        "fit_bias_two": normal_values(keys[12], (FIT,), 0.5, 3.0, jnp.float32),
        "fit_out": normal_values(keys[13], (FIT,), FIT ** -0.5, 0.5, jnp.float32),
    }


highest = lax.Precision.HIGHEST
radius_scale = 4.0
screen_width = 0.25
norm_floor = 1e-06
full_turn = 2.0 * math.pi

def stencil_table(anchor, weights, length, offset, periodic):
    count = anchor.shape[0]
    cell_index = lax.broadcasted_iota(jnp.int32, (4, length, count), 1)
    tap_index = lax.broadcasted_iota(jnp.int32, (4, length, count), 0)
    target = anchor[None, None, :] + tap_index + offset
    if periodic:
        target = target % length
    chosen = jnp.where(target == cell_index, weights[:, None, :], jnp.zeros((), weights.dtype))
    return lax.optimization_barrier(jnp.sum(chosen, axis=0))

def spread_cells(charge, anchor, weights, extent_x, extent_y, offset, length):
    table_x = stencil_table(anchor[0], weights[0] * charge[None, :], extent_x, offset, False)
    table_y = stencil_table(anchor[1], weights[1], extent_y, offset, False)
    table_z = stencil_table(anchor[2], weights[2], length, 0, True)
    planes = (table_x[:, None, :] * table_y[None, :, :]).reshape(extent_x * extent_y, -1)
    return jnp.dot(planes, table_z.T, precision=highest).reshape(extent_x, extent_y, length)

def interpolate(padded, anchor, weights, slopes):
    extent_x, extent_y, length = padded.shape
    table_x = stencil_table(anchor[0], weights[0], extent_x, 2, False)
    slope_x = stencil_table(anchor[0], slopes[0], extent_x, 2, False)
    table_y = stencil_table(anchor[1], weights[1], extent_y, 2, False)
    slope_y = stencil_table(anchor[1], slopes[1], extent_y, 2, False)
    table_z = stencil_table(anchor[2], weights[2], length, 0, True)
    slope_z = stencil_table(anchor[2], slopes[2], length, 0, True)
    flat = padded.reshape(extent_x * extent_y, length)
    along = jnp.dot(flat, table_z, precision=highest).reshape(extent_x, extent_y, -1)
    slant = jnp.dot(flat, slope_z, precision=highest).reshape(extent_x, extent_y, -1)
    over_y = lax.optimization_barrier(jnp.sum(along * table_y[None], axis=1))
    value = lax.optimization_barrier(jnp.sum(table_x * over_y, axis=0))
    field_x = -lax.optimization_barrier(jnp.sum(slope_x * over_y, axis=0))
    over_x = lax.optimization_barrier(jnp.sum(along * table_x[:, None, :], axis=0))
    field_y = -lax.optimization_barrier(jnp.sum(slope_y * over_x, axis=0))
    slant_y = lax.optimization_barrier(jnp.sum(slant * table_y[None], axis=1))
    field_z = -lax.optimization_barrier(jnp.sum(table_x * slant_y, axis=0))
    return (value, jnp.stack([field_x, field_y, field_z]))

def fitted_charge(nearby, listed, count, embed_scale, embed_bias, desc_gain, fit_in, fit_bias, fit_hidden, fit_bias_two, fit_out):
    atoms = listed.shape[1]
    center = nearby[:, 4 * atoms:5 * atoms]
    picked = jnp.take(nearby, listed.reshape(-1), axis=1).reshape(3, listed.shape[0], atoms)
    delta = picked - center[:, None, :]
    radius = jnp.sqrt(lax.optimization_barrier(jnp.sum(delta * delta, axis=0)))
    smooth = 1.0 / (1.0 + radius / radius_scale)
    factor = smooth / (radius + radius_scale)
    envelope = jnp.concatenate([smooth[None], delta * factor[None]], axis=0)
    embed = jnp.tanh(smooth[None] * embed_scale[:, None, None] + embed_bias[:, None, None])
    mixed = jnp.einsum('ekn,ckn->ecn', embed, envelope, precision=highest)
    descriptor = jnp.einsum('ecn,acn->ean', mixed, mixed[:AXIS], precision=highest).reshape(-1, atoms)
    scaling = lax.rsqrt(lax.optimization_barrier(jnp.mean(descriptor * descriptor, axis=0)) + norm_floor)
    normed = (descriptor * scaling[None, :] * desc_gain[:, None]).astype(jnp.bfloat16)
    first = jnp.tanh(jnp.dot(fit_in, normed, preferred_element_type=jnp.float32) + fit_bias[:, None])
    second = jnp.tanh(jnp.dot(fit_hidden, first.astype(jnp.bfloat16), preferred_element_type=jnp.float32) + fit_bias_two[:, None]) + first
    charge = lax.optimization_barrier(jnp.sum(fit_out[:, None] * second, axis=0))
    slot_index = lax.broadcasted_iota(jnp.int32, (atoms,), 0)
    return jnp.where(slot_index < count, charge, jnp.zeros((), charge.dtype))

def wave_number(index, length):
    signed = jnp.where(index > length // 2, index - length, index)
    return signed.astype(jnp.float32) * (full_turn / length)

def green_values(index_x, index_y, index_z, length):
    wave_x = wave_number(index_x, length)
    wave_y = wave_number(index_y, length)
    wave_z = wave_number(index_z, length)
    square = wave_x * wave_x + wave_y * wave_y + wave_z * wave_z
    safe = jnp.where(square > 0, square, 1.0)
    value = 2.0 * full_turn * jnp.exp(-0.5 * screen_width * screen_width * square) / safe
    keep = (square > 0) & (index_z != length // 2)
    return jnp.where(keep, value, 0.0)

def fold_edges(padded, length):
    inner = padded[2:length + 2]
    inner = inner.at[0:2].add(padded[length + 2:length + 4])
    inner = inner.at[length - 2:length].add(padded[0:2])
    return inner

def reference(positions, neighbours, live_count, stencil_base, spline_weight, spline_slope, embed_scale, embed_bias, desc_gain, fit_in, fit_bias, fit_hidden, fit_bias_two, fit_out):
    blocks = []
    for stride_x in (-1, 0, 1):
        for stride_y in (-1, 0, 1):
            moved = jnp.roll(positions, (-stride_x, -stride_y), axis=(1, 2))
            offset = jnp.array([stride_x * CX, stride_y * CY, 0], dtype=positions.dtype)
            blocks.append(moved + offset[:, None, None, None])
    stacked = jnp.stack(blocks, axis=1)
    nearby = jnp.transpose(stacked, (2, 3, 0, 1, 4)).reshape(N_GX, N_GY, 3, 9 * ATOM_DEV)
    listed = jnp.transpose(neighbours, (1, 2, 0, 3))

    def one_column(nearby_one, listed_one, count_one):
        return fitted_charge(nearby_one, listed_one, count_one, embed_scale, embed_bias, desc_gain, fit_in, fit_bias, fit_hidden, fit_bias_two, fit_out)

    def one_row(items):
        return jax.vmap(one_column)(items[0], items[1], items[2])
    charges = lax.map(one_row, (nearby, listed, live_count))
    anchors = jnp.transpose(stencil_base, (1, 2, 0, 3))
    weights = jnp.transpose(spline_weight, (2, 3, 0, 1, 4))
    slopes = jnp.transpose(spline_slope, (2, 3, 0, 1, 4))

    def place(index, grid):
        row_index = (index // N_GY).astype(jnp.int32)
        col_index = (index % N_GY).astype(jnp.int32)
        cells = spread_cells(charges[row_index, col_index], anchors[row_index, col_index], weights[row_index, col_index], CX + 4, CY + 4, 2, GRID)
        start = (row_index * CX, col_index * CY, jnp.zeros((), jnp.int32))
        before = lax.dynamic_slice(grid, start, cells.shape)
        return lax.dynamic_update_slice(grid, before + cells, start)
    grid = lax.fori_loop(0, N_GX * N_GY, place, jnp.zeros((GRID + 4, GRID + 4, GRID), jnp.float32))
    grid = fold_edges(grid, GRID)
    density = jnp.swapaxes(fold_edges(jnp.swapaxes(grid, 0, 1), GRID), 0, 1)
    modes = jnp.arange(GRID, dtype=jnp.int32)
    green = green_values(modes[:, None, None], modes[None, :, None], modes[None, None, :], GRID)
    spectrum = jnp.fft.fftn(density) * green
    potential = jnp.real(jnp.fft.ifftn(spectrum)).astype(jnp.float32)
    padded = jnp.pad(potential, ((2, 2), (2, 2), (0, 0)), mode='wrap')

    def gather_one(index):
        row_index = (index // N_GY).astype(jnp.int32)
        col_index = (index % N_GY).astype(jnp.int32)
        start = (row_index * CX, col_index * CY, jnp.zeros((), jnp.int32))
        window = lax.dynamic_slice(padded, start, (CX + 4, CY + 4, GRID))
        value, field = interpolate(window, anchors[row_index, col_index], weights[row_index, col_index], slopes[row_index, col_index])
        charge = charges[row_index, col_index]
        return (0.5 * charge * value, charge[None, :] * field)
    energy, force = lax.map(gather_one, jnp.arange(N_GX * N_GY, dtype=jnp.int32))
    energy = energy.reshape(N_GX, N_GY, ATOM_DEV)
    force = jnp.transpose(force.reshape(N_GX, N_GY, 3, ATOM_DEV), (2, 0, 1, 3))
    return (energy, force)
```

```python
import math

import jax
import jax.numpy as jnp
from jax import lax
from jax.experimental import pallas as pl
from jax.experimental.pallas import tpu as pltpu
from jax.sharding import PartitionSpec as P

GRID = 384
AXIS = 16
LANES = 128
CHUNK = 512
TILE = 256
FINE = (5, 13)

highest = lax.Precision.HIGHEST
radius_scale = 4.0
screen_width = 0.25
norm_floor = 1e-06
full_turn = 2.0 * math.pi


def peer_place(index, rows):
    return (index // rows, index % rows)


def greet_peers(me, peers, rows):
    barrier = pltpu.get_barrier_semaphore()

    def greet(k, carry):
        pl.semaphore_signal(
            barrier,
            inc=1,
            device_id=peer_place((me + k) % peers, rows),
            device_id_type=pl.DeviceIdType.MESH,
        )
        return carry

    lax.fori_loop(1, peers, greet, 0)
    return barrier


def column(table, index, length):
    return jnp.broadcast_to(table[:length, index : index + 1], (length, LANES))


def site_kernel(
    position_ref,
    neighbour_ref,
    count_ref,
    base_ref,
    slope_ref,
    scale_ref,
    bias_ref,
    gain_ref,
    fit_in_ref,
    fit_bias_ref,
    fit_hidden_ref,
    fit_bias_two_ref,
    fit_out_ref,
    sites_ref,
    charges_ref,
    counts_ref,
    place_ref,
    parcel_ref,
    own_ref,
    near_ref,
    listed_ref,
    rows_ref,
    columns_ref,
    gains_ref,
    env_ref,
    mixed_ref,
    descriptor_ref,
    normed_ref,
    near_send,
    near_recv,
    site_send,
    site_recv,
    charge_send,
    charge_recv,
):
    size_x = lax.axis_size("gx")
    size_y = lax.axis_size("gy")
    peers = size_x * size_y
    place_x = lax.axis_index("gx")
    place_y = lax.axis_index("gy")
    me = place_x * size_y + place_y
    width_x = GRID // size_x
    width_y = GRID // size_y
    neigh = neighbour_ref.shape[0]
    atoms = neighbour_ref.shape[3]
    width = scale_ref.shape[1]
    features = gain_ref.shape[1]
    barrier = greet_peers(me, peers, size_y)

    count = count_ref[0, 0]
    origin = (place_x * width_x + 1, place_y * width_y + 1, 1)
    place_ref[...] = jnp.zeros_like(place_ref)
    parcel_ref[...] = jnp.zeros_like(parcel_ref)
    for c in range(3):
        place_ref[c : c + 1, :] = position_ref[c, 0]
        parcel_ref[c : c + 1, :] = (base_ref[c, 0] + origin[c]).astype(jnp.float32)
        parcel_ref[c + 3 : c + 4, :] = slope_ref[c, 0, 0] + slope_ref[c, 3, 0] + 0.5
    parcel_ref[6:7, :] = jnp.full((1, atoms), count, jnp.int32).astype(jnp.float32)
    for k in range(neigh):
        listed_ref[k : k + 1, :] = neighbour_ref[k, 0]

    pl.semaphore_wait(barrier, peers - 1)

    def near_copy(slot, target):
        return pltpu.make_async_remote_copy(
            src_ref=place_ref,
            dst_ref=near_ref.at[slot],
            send_sem=near_send.at[slot],
            recv_sem=near_recv.at[slot],
            device_id=target,
            device_id_type=pl.DeviceIdType.MESH,
        )

    around = [(a, b) for a in (-1, 0, 1) for b in (-1, 0, 1)]
    targets = [((place_x - a) % size_x, (place_y - b) % size_y) for a, b in around]
    for slot in range(9):
        if slot != 4:
            near_copy(slot, targets[slot]).start()

    def site_copy(k, place):
        return pltpu.make_async_remote_copy(
            src_ref=parcel_ref,
            dst_ref=sites_ref.at[place],
            send_sem=site_send.at[k],
            recv_sem=site_recv.at[place],
            device_id=peer_place((me + k) % peers, size_y),
            device_id_type=pl.DeviceIdType.MESH,
        )

    def site_start(k, carry):
        site_copy(k, me).start()
        return carry

    lax.fori_loop(1, peers, site_start, 0)
    near_ref[4] = place_ref[...]
    sites_ref[me] = parcel_ref[...]

    rows_ref[...] = jnp.zeros_like(rows_ref)
    for index, ref in enumerate((scale_ref, bias_ref)):
        rows_ref[index : index + 1, :width] = ref[...]
    for index, ref in enumerate((fit_bias_ref, fit_bias_two_ref, fit_out_ref)):
        rows_ref[index + 2 : index + 3, :] = ref[...]
    parts = -(-features // LANES)
    for part in range(parts):
        size = min(LANES, features - part * LANES)
        rows_ref[part + 5 : part + 6, :size] = gain_ref[:, part * LANES : part * LANES + size]
    columns_ref[...] = rows_ref[...].T
    for part in range(parts):
        size = min(LANES, features - part * LANES)
        gains_ref[part * LANES : part * LANES + size, :] = column(columns_ref, part + 5, size)

    for slot in range(9):
        if slot != 4:
            near_copy(slot, targets[slot]).wait_send()
            near_copy(slot, targets[slot]).wait_recv()

    listed = listed_ref[...]
    slots = listed % atoms
    blocks = listed // atoms
    square = jnp.zeros((neigh, atoms), jnp.float32)
    deltas = []
    for c in range(3):
        center = near_ref[4, c : c + 1, :]
        picked = jnp.zeros((neigh, atoms), jnp.float32)
        for slot, (a, b) in enumerate(around):
            offset = (a * width_x, b * width_y, 0)[c]
            row = jnp.broadcast_to(near_ref[slot, c : c + 1, :] + float(offset), (neigh, atoms))
            got = jnp.take_along_axis(row, slots, axis=1, mode="promise_in_bounds")
            picked = jnp.where(blocks == slot, got, picked)
        delta = picked - center
        deltas.append(delta)
        square = square + delta * delta
    radius = jnp.sqrt(square)
    smooth = 1.0 / (1.0 + radius / radius_scale)
    factor = smooth / (radius + radius_scale)
    env_ref[0] = smooth
    for c in range(3):
        env_ref[c + 1] = deltas[c] * factor

    padded = mixed_ref.shape[1]
    bounds = [(0, padded // 16 * 8), (padded // 16 * 8, padded)]
    for first, last in bounds:
        span = last - first
        scale = jnp.broadcast_to(columns_ref[first:last, 0:1], (span, atoms))
        shift = jnp.broadcast_to(columns_ref[first:last, 1:2], (span, atoms))

        def step(k, sums):
            rows = [env_ref[c, pl.ds(k, 1), :] for c in range(4)]
            embed = jnp.tanh(rows[0] * scale + shift)
            return tuple(total + embed * row for total, row in zip(sums, rows))

        zero = jnp.zeros((span, atoms), jnp.float32)
        sums = lax.fori_loop(0, neigh, step, (zero, zero, zero, zero))
        for c in range(4):
            mixed_ref[c, first:last, :] = sums[c]

    def describe(e, total):
        value = jnp.zeros((AXIS, atoms), jnp.float32)
        for c in range(4):
            value = value + mixed_ref[c, pl.ds(e, 1), :] * mixed_ref[c, :AXIS, :]
        descriptor_ref[pl.ds(pl.multiple_of(e * AXIS, AXIS), AXIS), :] = value
        return total + value * value

    total = lax.fori_loop(0, width, describe, jnp.zeros((AXIS, atoms), jnp.float32), unroll=4)
    mean = jnp.sum(total, axis=0, keepdims=True) / features
    scaling = lax.rsqrt(mean + norm_floor)
    normed_ref[...] = (descriptor_ref[...] * scaling * gains_ref[...]).astype(jnp.bfloat16)
    whole = features // LANES * LANES
    first = jnp.dot(
        fit_in_ref[:, :whole], normed_ref[:whole, :], preferred_element_type=jnp.float32
    )
    if whole < features:
        first = first + jnp.dot(
            fit_in_ref[:, whole:], normed_ref[whole:, :], preferred_element_type=jnp.float32
        )
    first = jnp.tanh(first + column(columns_ref, 2, LANES))
    second = jnp.dot(
        fit_hidden_ref[...], first.astype(jnp.bfloat16), preferred_element_type=jnp.float32
    )
    second = jnp.tanh(second + column(columns_ref, 3, LANES)) + first
    charge = jnp.sum(column(columns_ref, 4, LANES) * second, axis=0, keepdims=True)
    lane = lax.broadcasted_iota(jnp.int32, (1, atoms), 1)
    own_ref[...] = jnp.where(lane < count, charge, 0.0)

    def site_land(k, carry):
        site_copy(k, me).wait_send()
        site_copy(k, (me + k) % peers).wait_recv()
        return carry

    lax.fori_loop(1, peers, site_land, 0)

    def charge_copy(k, place):
        return pltpu.make_async_remote_copy(
            src_ref=own_ref,
            dst_ref=charges_ref.at[place],
            send_sem=charge_send.at[k],
            recv_sem=charge_recv.at[place],
            device_id=peer_place((me + k) % peers, size_y),
            device_id_type=pl.DeviceIdType.MESH,
        )

    def charge_start(k, carry):
        charge_copy(k, me).start()
        return carry

    lax.fori_loop(1, peers, charge_start, 0)
    charges_ref[me] = own_ref[...]

    def tally(p, carry):
        counts_ref[pl.ds(p, 1), :] = sites_ref[p, 6:7, :].astype(jnp.int32)
        return carry

    lax.fori_loop(0, peers, tally, 0)

    def charge_land(k, carry):
        charge_copy(k, me).wait_send()
        charge_copy(k, (me + k) % peers).wait_recv()
        return carry

    lax.fori_loop(1, peers, charge_land, 0)


def gathered_sites(collective, *args):
    peers = lax.axis_size("gx") * lax.axis_size("gy")
    neigh = args[1].shape[0]
    atoms = args[1].shape[3]
    width = args[5].shape[1]
    features = args[7].shape[1]
    padded = -(-width // 8) * 8
    vmem = pl.BlockSpec(memory_space=pltpu.VMEM)
    smem = pl.BlockSpec(memory_space=pltpu.SMEM)
    dma = pltpu.SemaphoreType.DMA
    return pl.pallas_call(
        site_kernel,
        in_specs=[vmem, vmem, smem] + [vmem] * 10,
        out_specs=(vmem, vmem, vmem),
        out_shape=(
            jax.ShapeDtypeStruct((peers, 8, atoms), jnp.float32),
            jax.ShapeDtypeStruct((peers, 1, atoms), jnp.float32),
            jax.ShapeDtypeStruct((peers, atoms), jnp.int32),
        ),
        scratch_shapes=[
            pltpu.VMEM((8, atoms), jnp.float32),
            pltpu.VMEM((8, atoms), jnp.float32),
            pltpu.VMEM((1, atoms), jnp.float32),
            pltpu.VMEM((9, 8, atoms), jnp.float32),
            pltpu.VMEM((neigh, atoms), jnp.int32),
            pltpu.VMEM((LANES, LANES), jnp.float32),
            pltpu.VMEM((LANES, LANES), jnp.float32),
            pltpu.VMEM((features, atoms), jnp.float32),
            pltpu.VMEM((4, neigh, atoms), jnp.float32),
            pltpu.VMEM((4, padded, atoms), jnp.float32),
            pltpu.VMEM((features, atoms), jnp.float32),
            pltpu.VMEM((features, atoms), jnp.bfloat16),
            dma((9,)),
            dma((9,)),
            dma((peers,)),
            dma((peers,)),
            dma((peers,)),
            dma((peers,)),
        ],
        compiler_params=pltpu.CompilerParams(collective_id=collective, has_side_effects=True),
    )(*args)


def sine(index):
    angle = index * (full_turn / GRID)
    square = angle * angle
    total = jnp.full_like(square, -1.0 / 39916800.0)
    for term in (1.0 / 362880.0, -1.0 / 5040.0, 1.0 / 120.0, -1.0 / 6.0, 1.0):
        total = total * square + term
    return total * angle


def turned(index):
    index = index - GRID * jnp.floor(index * (1.0 / GRID))
    signed = index - GRID // 2
    size = jnp.abs(signed)
    near = jnp.minimum(size, GRID // 2 - size)
    return sine(size - GRID // 4), sine(jnp.where(signed < 0, near, -near))


def spline_taps(part):
    rest = 1.0 - part
    square = part * part
    cube = square * part
    weights = (
        rest * rest * rest * (1.0 / 6.0),
        (3.0 * cube - 6.0 * square + 4.0) * (1.0 / 6.0),
        (-3.0 * cube + 3.0 * square + 3.0 * part + 1.0) * (1.0 / 6.0),
        cube * (1.0 / 6.0),
    )
    slopes = (
        -0.5 * rest * rest,
        (3.0 * square - 4.0 * part) * 0.5,
        (-3.0 * square + 2.0 * part + 1.0) * 0.5,
        0.5 * square,
    )
    return weights, slopes


def mode_pairs(taps, wave):
    (cos_one, sin_one, cos_two, sin_two), (cosine, sine_part) = wave
    real = taps[1] + (taps[0] + taps[2]) * cos_one + taps[3] * cos_two
    imag = (taps[2] - taps[0]) * sin_one + taps[3] * sin_two
    return cosine * real - sine_part * imag, sine_part * real + cosine * imag


def field_kernel(
    sites_ref,
    charges_ref,
    listed_ref,
    out_ref,
    count_ref,
    packed_ref,
    wave_ref,
    high_ref,
    x_ref,
    slope_x_ref,
    y_ref,
    slope_y_ref,
    lit_ref,
    z_ref,
    slope_z_ref,
    plane_ref,
    weight_ref,
    row_ref,
    spectrum_ref,
    scaled_ref,
    found_ref,
    sem,
):
    size_x = lax.axis_size("gx")
    size_y = lax.axis_size("gy")
    columns = size_x * size_y
    modes_x = x_ref.shape[0]
    modes_y = y_ref.shape[0]
    modes_z = spectrum_ref.shape[1]
    half_x = modes_x // 2
    half_y = modes_y // 2
    half_z = modes_z // 2
    start_x = lax.axis_index("gx") * half_x
    start_y = lax.axis_index("gy") * half_y
    group = 8
    shape = (8, LANES)
    copy = pltpu.make_async_copy(listed_ref, count_ref, sem)
    copy.start()

    spectrum_ref[...] = jnp.zeros_like(spectrum_ref)
    found_ref[...] = jnp.zeros_like(found_ref)
    packed_ref[...] = jnp.zeros_like(packed_ref)
    sub = lax.broadcasted_iota(jnp.int32, shape, 0).astype(jnp.float32)
    lane = lax.broadcasted_iota(jnp.int32, shape, 1)
    starts = [start_x.astype(jnp.float32), start_y.astype(jnp.float32), 0.0]
    groups = [half_x // 8, half_y // 8, half_z // 8]
    firsts = [0, groups[0], groups[0] + groups[1]]
    for d in range(3):

        def waves(g, carry):
            mode = sub + (starts[d] + 8.0 * g.astype(jnp.float32))
            one = turned(mode)
            two = turned(2.0 * mode)
            for index, value in enumerate(one + two):
                wave_ref[firsts[d] + g, index] = value
            return carry

        lax.fori_loop(0, groups[d], waves, 0)

    fine = LANES // 2
    spot = lax.broadcasted_iota(jnp.int32, (modes_y, modes_z), 1)
    rest = jnp.where(spot < LANES, spot, (spot - LANES) % (half_z - fine))
    mode = jnp.where(
        spot < LANES, FINE[0] * 8 + spot % fine, jnp.where(rest < FINE[0] * 8, rest, rest + fine)
    ).astype(jnp.float32)
    factor = jnp.where(mode == 0, 1.0, 2.0) * (1.0 / GRID)
    wave = mode * (full_turn / GRID)
    square = wave * wave
    spot = lax.broadcasted_iota(jnp.int32, (modes_y, modes_z), 0)
    mode = start_y + jnp.where(spot < half_y, spot, spot - half_y)
    mode = jnp.where((mode == 0) & (spot >= half_y), GRID // 2, mode)
    ends = (mode == 0) | (mode == GRID // 2)
    factor = factor * jnp.where(ends, 1.0, 2.0) * (1.0 / GRID)
    wave = mode.astype(jnp.float32) * (full_turn / GRID)
    square = square + wave * wave
    decay = -0.5 * screen_width * screen_width
    plane_ref[...] = square
    weight_ref[...] = jnp.exp(square * decay) * factor * (2.0 * full_turn)
    spot = lax.broadcasted_iota(jnp.int32, (modes_x, LANES), 0)
    mode = start_x + jnp.where(spot < half_x, spot, spot - half_x)
    mode = jnp.where((mode == 0) & (spot >= half_x), GRID // 2, mode)
    ends = (mode == 0) | (mode == GRID // 2)
    wave = mode.astype(jnp.float32) * (full_turn / GRID)
    square = wave * wave
    row_ref[0] = square
    row_ref[1] = jnp.exp(square * decay) * jnp.where(ends, 1.0, 2.0) * (1.0 / GRID)

    copy.wait()

    def pack(j, start):
        count = count_ref[j, 0]
        tile = start // LANES
        shift = start % LANES
        site = jnp.where(
            lax.broadcasted_iota(jnp.int32, shape, 0) == 7,
            jnp.broadcast_to(charges_ref[j], shape),
            sites_ref[j],
        )
        turn = pltpu.roll(jnp.where(lane < count, site, 0.0), shift, 1)
        packed_ref[tile] = packed_ref[tile] + jnp.where(lane >= shift, turn, 0.0)
        packed_ref[tile + 1] = jnp.where(lane < shift, turn, 0.0)
        return start + count

    total = lax.fori_loop(0, columns, pack, 0)
    chunks = (total + CHUNK - 1) // CHUNK
    order = list(range(*FINE)) + list(range(FINE[0])) + list(range(FINE[1], groups[2]))

    def tables(tile, carry):
        lanes = pl.ds(pl.multiple_of(tile * LANES, LANES), LANES)
        charge = jnp.broadcast_to(packed_ref[tile, 7:8, :], shape)
        for d in range(3):
            cell = jnp.broadcast_to(packed_ref[tile, d : d + 1, :], shape)
            part = jnp.broadcast_to(packed_ref[tile, d + 3 : d + 4, :], shape)
            weights, slopes = spline_taps(part)
            low_cos, low_sin = turned(sub * cell)
            for h in range(-(-groups[d] // 8)):
                high_cos, high_sin = turned((starts[d] + 8.0 * (sub + 8.0 * h)) * cell)
                high_ref[0, 8 * h : 8 * h + 8] = high_cos
                high_ref[1, 8 * h : 8 * h + 8] = high_sin

            def pairs(g):
                high_cos = high_ref[0, g : g + 1]
                high_sin = high_ref[1, g : g + 1]
                constants = tuple(wave_ref[firsts[d] + g, index] for index in range(4))
                wave = (
                    constants,
                    (
                        high_cos * low_cos - high_sin * low_sin,
                        high_sin * low_cos + high_cos * low_sin,
                    ),
                )
                return mode_pairs(weights, wave) + mode_pairs(slopes, wave)

            if d < 2:
                half = groups[d] * 8
                for g in range(groups[d]):
                    even, odd, slope_even, slope_odd = pairs(g)
                    if g == 0:
                        parity = cell - 2.0 * jnp.floor(cell * 0.5)
                        parity = 1.0 - 2.0 * parity
                        first = (sub + starts[d]) == 0
                        last = parity * (weights[1] + weights[3] - weights[0] - weights[2])
                        odd = jnp.where(first, last, odd)
                        last = parity * (slopes[1] + slopes[3] - slopes[0] - slopes[2])
                        slope_odd = jnp.where(first, last, slope_odd)
                    table = (x_ref, y_ref)[d]
                    slope = (slope_x_ref, slope_y_ref)[d]
                    table[8 * g : 8 * g + 8, lanes] = even
                    table[half + 8 * g : half + 8 * g + 8, lanes] = odd
                    slope[8 * g : 8 * g + 8, lanes] = slope_even
                    slope[half + 8 * g : half + 8 * g + 8, lanes] = slope_odd
                    if d == 1:
                        lit_ref[8 * g : 8 * g + 8, lanes] = even * charge
                        lit_ref[half + 8 * g : half + 8 * g + 8, lanes] = odd * charge
                continue
            for index in range(0, len(order), 2):
                both = [pairs(order[index]), pairs(order[index + 1])]
                fine_part = index < FINE[1] - FINE[0]
                if fine_part:
                    spots = (8 * index, fine + 8 * index)
                else:
                    spots = (LANES + 8 * index - fine, half_z + 8 * index)
                for which in range(4):
                    table = z_ref if which < 2 else slope_z_ref
                    value = jnp.concatenate([both[0][which], both[1][which]], axis=0)
                    high = value.astype(jnp.bfloat16)
                    row = spots[which % 2]
                    table[row : row + 16, lanes] = high
                    if fine_part:
                        low = value - high.astype(jnp.float32)
                        row = row + modes_z
                        table[row : row + 16, lanes] = low.astype(jnp.bfloat16)
        return carry

    lax.fori_loop(0, chunks * (CHUNK // LANES), tables, 0)

    def gather_chunk(chunk, carry):
        lanes = pl.ds(pl.multiple_of(chunk * CHUNK, CHUNK), CHUNK)
        y = lit_ref[:, lanes]
        z = z_ref[:, lanes]

        def rows(g, inner):
            x = x_ref[pl.ds(pl.multiple_of(g * group, group), group), lanes]
            left = jnp.concatenate(
                [(x[a : a + 1] * y).astype(jnp.bfloat16) for a in range(group)], axis=0
            )
            where = pl.ds(pl.multiple_of(g * group * modes_y, group * modes_y), group * modes_y)
            form = (((1,), (1,)), ((), ()))
            both = lax.dot_general(left, z, form, preferred_element_type=jnp.float32)
            spectrum_ref[where, :LANES] += both[:, :LANES] + both[:, modes_z:]
            spectrum_ref[where, LANES:] += both[:, LANES:modes_z]
            return inner

        return lax.fori_loop(0, modes_x // group, rows, carry)

    lax.fori_loop(0, chunks, gather_chunk, 0)

    def scale(a, carry):
        def spread(ref, width):
            row = ref[pl.ds(a, 1), :]
            return jnp.concatenate([row] * (width // LANES), axis=1)

        square = plane_ref[...] + spread(row_ref.at[0], modes_z)
        safe = jnp.where(square > 0, square, 1.0)
        green = jnp.where(square > 0, weight_ref[...], 0.0) / safe * spread(row_ref.at[1], modes_z)
        where = pl.ds(pl.multiple_of(a * modes_y, modes_y), modes_y)
        value = (spectrum_ref[where, :] * green).astype(jnp.bfloat16)
        scaled_ref[where, :modes_z] = value
        scaled_ref[where, modes_z:] = value[:, :LANES]
        return carry

    lax.fori_loop(0, modes_x, scale, 0)

    def tile_step(tile, carry):
        lanes = pl.ds(pl.multiple_of(tile * TILE, TILE), TILE)
        y = y_ref[:, lanes]
        slope_y = slope_y_ref[:, lanes]
        z = z_ref[:, lanes]
        slope_z = slope_z_ref[:, lanes]

        def rows(g, sums):
            spot = pl.ds(pl.multiple_of(g * group, group), group)
            x = x_ref[spot, lanes]
            slope_x = slope_x_ref[spot, lanes]
            where = pl.ds(pl.multiple_of(g * group * modes_y, group * modes_y), group * modes_y)
            left = scaled_ref[where, :]
            along = jnp.dot(left, z, preferred_element_type=jnp.float32)
            slant = jnp.dot(left, slope_z, preferred_element_type=jnp.float32)
            value, field_x, field_y, field_z = sums
            for a in range(group):
                part = along[a * modes_y : (a + 1) * modes_y]
                skew = slant[a * modes_y : (a + 1) * modes_y]
                over = jnp.sum((part * y).reshape(modes_y // 8, 8, TILE), axis=0)
                tilt = jnp.sum((part * slope_y).reshape(modes_y // 8, 8, TILE), axis=0)
                deep = jnp.sum((skew * y).reshape(modes_y // 8, 8, TILE), axis=0)
                row = x[a : a + 1]
                value = value + over * row
                field_x = field_x + over * slope_x[a : a + 1]
                field_y = field_y + tilt * row
                field_z = field_z + deep * row
            return value, field_x, field_y, field_z

        zero = jnp.zeros((8, TILE), jnp.float32)
        sums = lax.fori_loop(0, modes_x // group, rows, (zero, zero, zero, zero))
        for part in range(TILE // LANES):
            for c in range(4):
                found_ref[tile * (TILE // LANES) + part, c : c + 1, :] = jnp.sum(
                    sums[c][:, part * LANES : (part + 1) * LANES], axis=0, keepdims=True
                )
        return carry

    lax.fori_loop(0, (total + TILE - 1) // TILE, tile_step, 0)

    def place(j, start):
        tile = start // LANES
        shift = start % LANES
        back = (LANES - shift) % LANES
        first = pltpu.roll(found_ref[tile], back, 1)
        second = pltpu.roll(found_ref[tile + 1], back, 1)
        out_ref[j] = jnp.where(lane < LANES - shift, first, second)[:4]
        return start + count_ref[j, 0]

    lax.fori_loop(0, columns, place, 0)


def mesh_sums(sites, charges, counts):
    size_x = lax.axis_size("gx")
    size_y = lax.axis_size("gy")
    columns, _, atoms = sites.shape
    slots = -(-(columns * atoms) // CHUNK) * CHUNK
    modes_x = GRID // size_x
    modes_y = GRID // size_y
    groups = (modes_x + modes_y + GRID) // 16
    vmem = pl.BlockSpec(memory_space=pltpu.VMEM)
    table = lambda rows: pltpu.VMEM((rows, slots), jnp.float32)
    return pl.pallas_call(
        field_kernel,
        in_specs=[vmem, vmem, vmem],
        out_specs=vmem,
        out_shape=jax.ShapeDtypeStruct((columns, 4, atoms), jnp.float32),
        scratch_shapes=[
            pltpu.SMEM(counts.shape, jnp.int32),
            pltpu.VMEM((slots // LANES + 2, 8, LANES), jnp.float32),
            pltpu.VMEM((groups, 4, 8, LANES), jnp.float32),
            pltpu.VMEM((2, 24, LANES), jnp.float32),
            table(modes_x),
            table(modes_x),
            table(modes_y),
            table(modes_y),
            table(modes_y),
            pltpu.VMEM((GRID + LANES, slots), jnp.bfloat16),
            pltpu.VMEM((GRID + LANES, slots), jnp.bfloat16),
            pltpu.VMEM((modes_y, GRID), jnp.float32),
            pltpu.VMEM((modes_y, GRID), jnp.float32),
            pltpu.VMEM((2, modes_x, LANES), jnp.float32),
            pltpu.VMEM((modes_x * modes_y, GRID), jnp.float32),
            pltpu.VMEM((modes_x * modes_y, GRID + LANES), jnp.bfloat16),
            pltpu.VMEM((slots // LANES + 2, 8, LANES), jnp.float32),
            pltpu.SemaphoreType.DMA,
        ],
        compiler_params=pltpu.CompilerParams(vmem_limit_bytes=60 * 2**20),
    )(sites, charges, counts)


def finish_kernel(sums_ref, charge_ref, out_ref, landed_ref, send_sem, recv_sem):
    rows = lax.axis_size("gy")
    peers = lax.axis_size("gx") * rows
    me = lax.axis_index("gx") * rows + lax.axis_index("gy")
    pl.semaphore_wait(greet_peers(me, peers, rows), peers - 1)

    def copy_to(k, place):
        peer = (me + k) % peers
        return pltpu.make_async_remote_copy(
            src_ref=sums_ref.at[peer],
            dst_ref=landed_ref.at[place],
            send_sem=send_sem.at[k],
            recv_sem=recv_sem.at[place],
            device_id=peer_place(peer, rows),
            device_id_type=pl.DeviceIdType.MESH,
        )

    def send(k, carry):
        copy_to(k, me).start()
        return carry

    lax.fori_loop(1, peers, send, 0)
    landed_ref[me] = sums_ref[me]

    def land(k, carry):
        copy_to(k, me).wait_send()
        copy_to(k, (me + k) % peers).wait_recv()
        return carry

    lax.fori_loop(1, peers, land, 0)
    total = jnp.sum(landed_ref[...], axis=0)
    charge = charge_ref[me]
    out_ref[0:1] = 0.5 * charge * total[0:1]
    out_ref[1:4] = -charge * total[1:4]


def finish(sums, charge, collective):
    peers, rows, atoms = sums.shape
    vmem = pl.BlockSpec(memory_space=pltpu.VMEM)
    return pl.pallas_call(
        finish_kernel,
        out_shape=jax.ShapeDtypeStruct((4, atoms), jnp.float32),
        in_specs=[vmem, vmem],
        out_specs=vmem,
        scratch_shapes=[
            pltpu.VMEM((peers, rows, atoms), jnp.float32),
            pltpu.SemaphoreType.DMA((peers,)),
            pltpu.SemaphoreType.DMA((peers,)),
        ],
        compiler_params=pltpu.CompilerParams(collective_id=collective, has_side_effects=True),
    )(sums, charge)


def local_sites(
    positions,
    neighbours,
    live_count,
    stencil_base,
    spline_weight,
    spline_slope,
    embed_scale,
    embed_bias,
    desc_gain,
    fit_in,
    fit_bias,
    fit_hidden,
    fit_bias_two,
    fit_out,
):
    atoms = positions.shape[3]
    sites, charges, counts = gathered_sites(
        1,
        positions,
        neighbours,
        live_count,
        stencil_base,
        spline_slope,
        embed_scale[None, :],
        embed_bias[None, :],
        desc_gain[None, :],
        fit_in,
        fit_bias[None, :],
        fit_hidden,
        fit_bias_two[None, :],
        fit_out[None, :],
    )
    mine = finish(mesh_sums(sites, charges, counts), charges, 2)
    energy = mine[0].reshape(1, 1, atoms)
    force = mine[1:].reshape(3, 1, 1, atoms)
    return (energy, force)


def padded_2(shard, sides, width):
    for axis, dim in sides:
        peers, length = (lax.axis_size(axis), shard.shape[dim])
        up = [(i, (i + 1) % peers) for i in range(peers)]
        down = [(j, i) for i, j in up]
        last = lax.slice_in_dim(shard, length - width, length, axis=dim)
        leading = lax.slice_in_dim(shard, 0, width, axis=dim)
        before = lax.ppermute(last, axis, up)
        after = lax.ppermute(leading, axis, down)
        shard = jnp.concatenate([before, shard, after], axis=dim)
    return shard


def shifted(block, axis, distance):
    devices = range(lax.axis_size(axis))
    route = [((i - distance) % len(devices), i) for i in devices]
    return lax.ppermute(block, axis, route)


def stencil_table(anchor, weights, length, offset, periodic):
    count = anchor.shape[0]
    cell_index = lax.broadcasted_iota(jnp.int32, (4, length, count), 1)
    tap_index = lax.broadcasted_iota(jnp.int32, (4, length, count), 0)
    target = anchor[None, None, :] + tap_index + offset
    if periodic:
        target = target % length
    chosen = jnp.where(target == cell_index, weights[:, None, :], jnp.zeros((), weights.dtype))
    return jnp.sum(chosen, axis=0)


def spread_cells(charge, anchor, weights, extent_x, extent_y, offset, length):
    table_x = stencil_table(anchor[0], weights[0] * charge[None, :], extent_x, offset, False)
    table_y = stencil_table(anchor[1], weights[1], extent_y, offset, False)
    table_z = stencil_table(anchor[2], weights[2], length, 0, True)
    planes = (table_x[:, None, :] * table_y[None, :, :]).reshape(extent_x * extent_y, -1)
    return jnp.dot(planes, table_z.T, precision=highest).reshape(extent_x, extent_y, length)


def interpolate(padded, anchor, weights, slopes):
    extent_x, extent_y, length = padded.shape
    table_x = stencil_table(anchor[0], weights[0], extent_x, 2, False)
    slope_x = stencil_table(anchor[0], slopes[0], extent_x, 2, False)
    table_y = stencil_table(anchor[1], weights[1], extent_y, 2, False)
    slope_y = stencil_table(anchor[1], slopes[1], extent_y, 2, False)
    table_z = stencil_table(anchor[2], weights[2], length, 0, True)
    slope_z = stencil_table(anchor[2], slopes[2], length, 0, True)
    flat = padded.reshape(extent_x * extent_y, length)
    along = jnp.dot(flat, table_z, precision=highest).reshape(extent_x, extent_y, -1)
    slant = jnp.dot(flat, slope_z, precision=highest).reshape(extent_x, extent_y, -1)
    over_y = jnp.sum(along * table_y[None], axis=1)
    value = jnp.sum(table_x * over_y, axis=0)
    field_x = -jnp.sum(slope_x * over_y, axis=0)
    over_x = jnp.sum(along * table_x[:, None, :], axis=0)
    field_y = -jnp.sum(slope_y * over_x, axis=0)
    slant_y = jnp.sum(slant * table_y[None], axis=1)
    field_z = -jnp.sum(table_x * slant_y, axis=0)
    return (value, jnp.stack([field_x, field_y, field_z]))


def fitted_charge(
    nearby,
    listed,
    count,
    embed_scale,
    embed_bias,
    desc_gain,
    fit_in,
    fit_bias,
    fit_hidden,
    fit_bias_two,
    fit_out,
):
    atoms = listed.shape[1]
    center = nearby[:, 4 * atoms : 5 * atoms]
    picked = jnp.take(nearby, listed.reshape(-1), axis=1).reshape(3, listed.shape[0], atoms)
    delta = picked - center[:, None, :]
    radius = jnp.sqrt(jnp.sum(delta * delta, axis=0))
    smooth = 1.0 / (1.0 + radius / radius_scale)
    factor = smooth / (radius + radius_scale)
    envelope = jnp.concatenate([smooth[None], delta * factor[None]], axis=0)
    embed = jnp.tanh(smooth[None] * embed_scale[:, None, None] + embed_bias[:, None, None])
    mixed = jnp.einsum("ekn,ckn->ecn", embed, envelope, precision=highest)
    descriptor = jnp.einsum("ecn,acn->ean", mixed, mixed[:AXIS], precision=highest).reshape(
        -1, atoms
    )
    scaling = lax.rsqrt(jnp.mean(descriptor * descriptor, axis=0) + norm_floor)
    normed = (descriptor * scaling[None, :] * desc_gain[:, None]).astype(jnp.bfloat16)
    first = jnp.tanh(
        jnp.dot(fit_in, normed, preferred_element_type=jnp.float32) + fit_bias[:, None]
    )
    second = (
        jnp.tanh(
            jnp.dot(fit_hidden, first.astype(jnp.bfloat16), preferred_element_type=jnp.float32)
            + fit_bias_two[:, None]
        )
        + first
    )
    charge = jnp.sum(fit_out[:, None] * second, axis=0)
    slot_index = lax.broadcasted_iota(jnp.int32, (atoms,), 0)
    return jnp.where(slot_index < count, charge, jnp.zeros((), charge.dtype))


def wave_number(index, length):
    signed = jnp.where(index > length // 2, index - length, index)
    return signed.astype(jnp.float32) * (full_turn / length)


def green_values(index_x, index_y, index_z, length):
    wave_x = wave_number(index_x, length)
    wave_y = wave_number(index_y, length)
    wave_z = wave_number(index_z, length)
    square = wave_x * wave_x + wave_y * wave_y + wave_z * wave_z
    safe = jnp.where(square > 0, square, 1.0)
    value = 2.0 * full_turn * jnp.exp(-0.5 * screen_width * screen_width * square) / safe
    keep = (square > 0) & (index_z != length // 2)
    return jnp.where(keep, value, 0.0)


def wave_tables(length, count):
    rows = lax.broadcasted_iota(jnp.int32, (length, count), 0)
    cols = lax.broadcasted_iota(jnp.int32, (length, count), 1)
    angle = (rows * cols % length).astype(jnp.float32) * (full_turn / length)
    return (jnp.cos(angle), jnp.sin(angle))


def along_axis(real_part, imag_part, cosine, sine, sign, form):
    real_cos = jnp.einsum(form, real_part, cosine, precision=highest)
    real_sin = jnp.einsum(form, real_part, sine, precision=highest)
    imag_cos = jnp.einsum(form, imag_part, cosine, precision=highest)
    imag_sin = jnp.einsum(form, imag_part, sine, precision=highest)
    return (real_cos + sign * imag_sin, imag_cos - sign * real_sin)


def local_mesh(
    positions,
    neighbours,
    live_count,
    stencil_base,
    spline_weight,
    spline_slope,
    embed_scale,
    embed_bias,
    desc_gain,
    fit_in,
    fit_bias,
    fit_hidden,
    fit_bias_two,
    fit_out,
):
    columns_y = lax.axis_size("gy")
    width_x = GRID // lax.axis_size("gx")
    width_y = GRID // columns_y
    atoms = positions.shape[3]
    beside_all = padded_2(positions, (("gx", 1), ("gy", 2)), 1)
    block_x = lax.broadcasted_iota(jnp.int32, (3, 3, atoms), 0) - 1
    block_y = lax.broadcasted_iota(jnp.int32, (3, 3, atoms), 1) - 1
    offsets = jnp.stack([block_x * width_x, block_y * width_y, jnp.zeros_like(block_x)]).astype(
        jnp.float32
    )
    nearby = (beside_all + offsets).reshape(3, 9 * atoms)
    charge = fitted_charge(
        nearby,
        neighbours[:, 0, 0, :],
        live_count[0, 0],
        embed_scale,
        embed_bias,
        desc_gain,
        fit_in,
        fit_bias,
        fit_hidden,
        fit_bias_two,
        fit_out,
    )
    anchor = stencil_base[:, 0, 0, :]
    weights = spline_weight[:, :, 0, 0, :]
    slopes = spline_slope[:, :, 0, 0, :]
    spread = spread_cells(charge, anchor, weights, width_x + 4, width_y + 4, 2, GRID)
    inner = spread[2 : width_x + 2]
    for stride in (1, -1):
        piece = spread[width_x + 2 :] if stride == 1 else spread[:2]
        moved = shifted(piece, "gx", stride)
        if stride == 1:
            inner = inner.at[:2].add(moved)
        else:
            inner = inner.at[width_x - 2 :].add(moved)
    density = inner[:, 2 : width_y + 2]
    for stride in (1, -1):
        piece = inner[:, width_y + 2 :] if stride == 1 else inner[:, :2]
        moved = shifted(piece, "gy", stride)
        if stride == 1:
            density = density.at[:, :2].add(moved)
        else:
            density = density.at[:, width_y - 2 :].add(moved)
    freqs = GRID // 2
    fold_weight = jnp.where(jnp.arange(freqs) == 0, 1.0, 2.0).astype(jnp.float32) / GRID
    cosine_z, sine_z = wave_tables(GRID, freqs)
    flat = density.reshape(width_x * width_y, GRID)
    real_part = jnp.dot(flat, cosine_z, precision=highest).reshape(width_x, width_y, freqs)
    imag_part = -jnp.dot(flat, sine_z, precision=highest).reshape(width_x, width_y, freqs)
    real_part, imag_part = (
        lax.all_to_all(real_part, "gy", split_axis=2, concat_axis=1, tiled=True),
        lax.all_to_all(imag_part, "gy", split_axis=2, concat_axis=1, tiled=True),
    )
    cosine, sine = wave_tables(GRID, GRID)
    real_part, imag_part = along_axis(real_part, imag_part, cosine, sine, 1.0, "xym,yk->xkm")
    real_part, imag_part = (
        lax.all_to_all(real_part, "gx", split_axis=1, concat_axis=0, tiled=True),
        lax.all_to_all(imag_part, "gx", split_axis=1, concat_axis=0, tiled=True),
    )
    real_part, imag_part = along_axis(real_part, imag_part, cosine, sine, 1.0, "xym,xk->kym")
    span_y = real_part.shape[1]
    span_z = real_part.shape[2]
    index_x = lax.broadcasted_iota(jnp.int32, (GRID, span_y, span_z), 0)
    index_y = lax.axis_index("gx") * span_y + lax.broadcasted_iota(
        jnp.int32, (GRID, span_y, span_z), 1
    )
    index_z = lax.axis_index("gy") * span_z + lax.broadcasted_iota(
        jnp.int32, (GRID, span_y, span_z), 2
    )
    green = green_values(index_x, index_y, index_z, GRID)
    real_part = real_part * green
    imag_part = imag_part * green
    back_cos = cosine / GRID
    back_sin = sine / GRID
    real_part, imag_part = along_axis(real_part, imag_part, back_cos, back_sin, -1.0, "xym,xk->kym")
    real_part, imag_part = (
        lax.all_to_all(real_part, "gx", split_axis=0, concat_axis=1, tiled=True),
        lax.all_to_all(imag_part, "gx", split_axis=0, concat_axis=1, tiled=True),
    )
    real_part, imag_part = along_axis(real_part, imag_part, back_cos, back_sin, -1.0, "xym,yk->xkm")
    real_part, imag_part = (
        lax.all_to_all(real_part, "gy", split_axis=1, concat_axis=2, tiled=True),
        lax.all_to_all(imag_part, "gy", split_axis=1, concat_axis=2, tiled=True),
    )
    rows_y = real_part.shape[1]
    flat_real = real_part.reshape(width_x * rows_y, freqs)
    flat_imag = imag_part.reshape(width_x * rows_y, freqs)
    summed_cos = (cosine_z * fold_weight[None, :]).T
    summed_sin = (sine_z * fold_weight[None, :]).T
    potential = jnp.dot(flat_real, summed_cos, precision=highest) - jnp.dot(
        flat_imag, summed_sin, precision=highest
    )
    potential = potential.reshape(width_x, rows_y, GRID)
    padded = padded_2(potential, (("gx", 0), ("gy", 1)), 2)
    value, field = interpolate(padded, anchor, weights, slopes)
    energy = (0.5 * charge * value).reshape(1, 1, atoms)
    force = (charge[None, :] * field).reshape(3, 1, 1, atoms)
    return (energy, force)


def solution(mesh):
    def local(positions, *rest):
        columns_x, columns_y = (lax.axis_size("gx"), lax.axis_size("gy"))
        sites = columns_x * columns_y * positions.shape[3]
        whole = GRID % (16 * columns_x) == 0 and GRID % (16 * columns_y) == 0
        few = whole and sites <= 8 * GRID * 2
        return (local_sites if few and positions.shape[3] == LANES else local_mesh)(positions, *rest)

    placed = (
        P(None, "gx", "gy", None),
        P(None, "gx", "gy", None),
        P("gx", "gy"),
        P(None, "gx", "gy", None),
        P(None, None, "gx", "gy", None),
        P(None, None, "gx", "gy", None),
        P(),
        P(),
        P(),
        P(),
        P(),
        P(),
        P(),
        P(),
    )
    return jax.shard_map(
        local,
        mesh=mesh,
        in_specs=placed,
        out_specs=(P("gx", "gy", None), P(None, "gx", "gy", None)),
        check_vma=False,
    )
```

```python
import math

import jax
import jax.numpy as jnp
from jax import lax
from jax.experimental import pallas as pl
from jax.experimental.pallas import tpu as pltpu
from jax.sharding import PartitionSpec as P

GRID = 384
AXIS = 16
LANES = 128
CHUNK = 256
TILE = 256
FINE = (5, 13)

highest = lax.Precision.HIGHEST
radius_scale = 4.0
screen_width = 0.25
norm_floor = 1e-06
full_turn = 2.0 * math.pi


def each_peer(visit):
    size_x = lax.axis_size("gx")
    size_y = lax.axis_size("gy")
    place_x = lax.axis_index("gx")
    place_y = lax.axis_index("gy")
    across = [(place_y + b) % size_y for b in range(size_y)]
    for b in range(1, size_y):
        visit(b, place_x, across[b])

    def row(a, carry):
        x = (place_x + a) % size_x
        for b in range(size_y):
            visit(a * size_y + b, x, across[b])
        return carry

    lax.fori_loop(1, size_x, row, 0)


def greet_peers():
    barrier = pltpu.get_barrier_semaphore()

    def greet(k, x, y):
        pl.semaphore_signal(
            barrier, inc=1, device_id=(x, y), device_id_type=pl.DeviceIdType.MESH
        )

    each_peer(greet)
    return barrier


def spread_piece(piece, whole_ref, send_sem, recv_sem):
    size_y = lax.axis_size("gy")
    me = lax.axis_index("gx") * size_y + lax.axis_index("gy")

    def copy(k, x, y, place):
        return pltpu.make_async_remote_copy(
            src_ref=piece(x * size_y + y),
            dst_ref=whole_ref.at[place],
            send_sem=send_sem.at[k],
            recv_sem=recv_sem.at[place],
            device_id=(x, y),
            device_id_type=pl.DeviceIdType.MESH,
        )

    def send(k, x, y):
        copy(k, x, y, me).start()

    def land(k, x, y):
        copy(k, x, y, me).wait_send()
        copy(k, x, y, x * size_y + y).wait_recv()

    return (lambda: each_peer(send)), (lambda: each_peer(land))


def column(table, index, length):
    return jnp.broadcast_to(table[:length, index : index + 1], (length, LANES))


def site_kernel(
    position_ref,
    neighbour_ref,
    count_ref,
    base_ref,
    slope_ref,
    scale_ref,
    bias_ref,
    gain_ref,
    fit_in_hbm,
    fit_bias_ref,
    fit_hidden_hbm,
    fit_bias_two_ref,
    fit_out_ref,
    sites_ref,
    charges_ref,
    counts_ref,
    place_ref,
    parcel_ref,
    own_ref,
    near_ref,
    listed_ref,
    rows_ref,
    columns_ref,
    gains_ref,
    env_ref,
    mixed_ref,
    descriptor_ref,
    normed_ref,
    fit_in_ref,
    fit_hidden_ref,
    load_sem,
    near_send,
    near_recv,
    site_send,
    site_recv,
    charge_send,
    charge_recv,
):
    size_x = lax.axis_size("gx")
    size_y = lax.axis_size("gy")
    peers = size_x * size_y
    place_x = lax.axis_index("gx")
    place_y = lax.axis_index("gy")
    me = place_x * size_y + place_y
    width_x = GRID // size_x
    width_y = GRID // size_y
    neigh = neighbour_ref.shape[0]
    atoms = neighbour_ref.shape[3]
    width = scale_ref.shape[1]
    features = gain_ref.shape[1]
    loads = [
        pltpu.make_async_copy(fit_in_hbm, fit_in_ref, load_sem.at[0]),
        pltpu.make_async_copy(fit_hidden_hbm, fit_hidden_ref, load_sem.at[1]),
    ]
    for load in loads:
        load.start()
    barrier = greet_peers()

    count = count_ref[0, 0]
    origin = (place_x * width_x + 1, place_y * width_y + 1, 1)
    place_ref[...] = jnp.zeros_like(place_ref)
    for c in range(3):
        place_ref[c : c + 1, :] = position_ref[c, 0]
        part = slope_ref[c, 0, 0] + slope_ref[c, 3, 0] + 0.5
        parcel_ref[c : c + 1, :] = (base_ref[c, 0] + origin[c]).astype(jnp.float32) + part
    parcel_ref[3:4, :] = jnp.full((1, atoms), count, jnp.int32).astype(jnp.float32)
    for k in range(neigh):
        listed_ref[k : k + 1, :] = neighbour_ref[k, 0]

    pl.semaphore_wait(barrier, peers - 1)

    def near_copy(slot, target):
        return pltpu.make_async_remote_copy(
            src_ref=place_ref,
            dst_ref=near_ref.at[slot],
            send_sem=near_send.at[slot],
            recv_sem=near_recv.at[slot],
            device_id=target,
            device_id_type=pl.DeviceIdType.MESH,
        )

    around = [(a, b) for a in (-1, 0, 1) for b in (-1, 0, 1)]
    targets = [((place_x - a) % size_x, (place_y - b) % size_y) for a, b in around]
    for slot in range(9):
        if slot != 4:
            near_copy(slot, targets[slot]).start()

    send_sites, land_sites = spread_piece(lambda p: parcel_ref, sites_ref, site_send, site_recv)
    send_sites()
    near_ref[4] = place_ref[...]
    sites_ref[me] = parcel_ref[...]

    rows_ref[...] = jnp.zeros_like(rows_ref)
    for index, ref in enumerate((scale_ref, bias_ref)):
        rows_ref[index : index + 1, :width] = ref[...]
    for index, ref in enumerate((fit_bias_ref, fit_bias_two_ref, fit_out_ref)):
        rows_ref[index + 2 : index + 3, :] = ref[...]
    parts = -(-features // LANES)
    for part in range(parts):
        size = min(LANES, features - part * LANES)
        rows_ref[part + 5 : part + 6, :size] = gain_ref[:, part * LANES : part * LANES + size]
    columns_ref[...] = rows_ref[...].T
    for part in range(parts):
        size = min(LANES, features - part * LANES)
        gains_ref[part * LANES : part * LANES + size, :] = column(columns_ref, part + 5, size)

    for slot in range(9):
        if slot != 4:
            near_copy(slot, targets[slot]).wait_send()
            near_copy(slot, targets[slot]).wait_recv()

    listed = listed_ref[...]
    slots = listed % atoms
    blocks = listed // atoms
    square = jnp.zeros((neigh, atoms), jnp.float32)
    deltas = []
    for c in range(3):
        center = near_ref[4, c : c + 1, :]
        picked = jnp.zeros((neigh, atoms), jnp.float32)
        for slot, (a, b) in enumerate(around):
            offset = (a * width_x, b * width_y, 0)[c]
            row = jnp.broadcast_to(near_ref[slot, c : c + 1, :] + float(offset), (neigh, atoms))
            got = jnp.take_along_axis(row, slots, axis=1, mode="promise_in_bounds")
            picked = jnp.where(blocks == slot, got, picked)
        delta = picked - center
        deltas.append(delta)
        square = square + delta * delta
    radius = jnp.sqrt(square)
    smooth = 1.0 / (1.0 + radius / radius_scale)
    factor = smooth / (radius + radius_scale)
    env_ref[0] = smooth
    for c in range(3):
        env_ref[c + 1] = deltas[c] * factor

    padded = mixed_ref.shape[1]
    bounds = [(0, padded // 16 * 8), (padded // 16 * 8, padded)]
    for first, last in bounds:
        span = last - first
        scale = jnp.broadcast_to(columns_ref[first:last, 0:1], (span, atoms))
        shift = jnp.broadcast_to(columns_ref[first:last, 1:2], (span, atoms))

        def step(k, sums):
            rows = [env_ref[c, pl.ds(k, 1), :] for c in range(4)]
            embed = jnp.tanh(rows[0] * scale + shift)
            return tuple(total + embed * row for total, row in zip(sums, rows))

        zero = jnp.zeros((span, atoms), jnp.float32)
        sums = lax.fori_loop(0, neigh, step, (zero, zero, zero, zero))
        for c in range(4):
            mixed_ref[c, first:last, :] = sums[c]

    def describe(e, total):
        value = jnp.zeros((AXIS, atoms), jnp.float32)
        for c in range(4):
            value = value + mixed_ref[c, pl.ds(e, 1), :] * mixed_ref[c, :AXIS, :]
        descriptor_ref[pl.ds(pl.multiple_of(e * AXIS, AXIS), AXIS), :] = value
        return total + value * value

    total = lax.fori_loop(0, width, describe, jnp.zeros((AXIS, atoms), jnp.float32), unroll=4)
    mean = jnp.sum(total, axis=0, keepdims=True) / features
    scaling = lax.rsqrt(mean + norm_floor)
    normed_ref[...] = (descriptor_ref[...] * scaling * gains_ref[...]).astype(jnp.bfloat16)
    for load in loads:
        load.wait()
    first = lax.dot_general(
        fit_in_ref[...],
        normed_ref[...],
        (((0,), (0,)), ((), ())),
        preferred_element_type=jnp.float32,
    )
    first = jnp.tanh(first + column(columns_ref, 2, LANES))
    second = jnp.dot(
        fit_hidden_ref[...], first.astype(jnp.bfloat16), preferred_element_type=jnp.float32
    )
    second = jnp.tanh(second + column(columns_ref, 3, LANES)) + first
    charge = jnp.sum(column(columns_ref, 4, LANES) * second, axis=0, keepdims=True)
    lane = lax.broadcasted_iota(jnp.int32, (1, atoms), 1)
    own_ref[...] = jnp.where(lane < count, charge, 0.0)

    send_charges, land_charges = spread_piece(
        lambda p: own_ref, charges_ref, charge_send, charge_recv
    )
    send_charges()
    charges_ref[me] = own_ref[...]
    land_sites()
    for p in range(peers):
        counts_ref[p : p + 1, :] = sites_ref[p, 3:4, :].astype(jnp.int32)
    land_charges()


def gathered_sites(collective, *args):
    peers = lax.axis_size("gx") * lax.axis_size("gy")
    neigh = args[1].shape[0]
    atoms = args[1].shape[3]
    width = args[5].shape[1]
    features = args[7].shape[1]
    padded = -(-width // 8) * 8
    vmem = pl.BlockSpec(memory_space=pltpu.VMEM)
    smem = pl.BlockSpec(memory_space=pltpu.SMEM)
    hbm = pl.BlockSpec(memory_space=pltpu.HBM)
    dma = pltpu.SemaphoreType.DMA
    return pl.pallas_call(
        site_kernel,
        in_specs=[vmem, vmem, smem] + [vmem] * 5 + [hbm, vmem, hbm, vmem, vmem],
        out_specs=(vmem, vmem, vmem),
        out_shape=(
            jax.ShapeDtypeStruct((peers, 4, atoms), jnp.float32),
            jax.ShapeDtypeStruct((peers, 1, atoms), jnp.float32),
            jax.ShapeDtypeStruct((peers, atoms), jnp.int32),
        ),
        scratch_shapes=[
            pltpu.VMEM((4, atoms), jnp.float32),
            pltpu.VMEM((4, atoms), jnp.float32),
            pltpu.VMEM((1, atoms), jnp.float32),
            pltpu.VMEM((9, 4, atoms), jnp.float32),
            pltpu.VMEM((neigh, atoms), jnp.int32),
            pltpu.VMEM((LANES, LANES), jnp.float32),
            pltpu.VMEM((LANES, LANES), jnp.float32),
            pltpu.VMEM((features, atoms), jnp.float32),
            pltpu.VMEM((4, neigh, atoms), jnp.float32),
            pltpu.VMEM((4, padded, atoms), jnp.float32),
            pltpu.VMEM((features, atoms), jnp.float32),
            pltpu.VMEM((features, atoms), jnp.bfloat16),
            pltpu.VMEM(args[8].shape, args[8].dtype),
            pltpu.VMEM(args[10].shape, args[10].dtype),
            dma((2,)),
            dma((9,)),
            dma((9,)),
            dma((peers,)),
            dma((peers,)),
            dma((peers,)),
            dma((peers,)),
        ],
        compiler_params=pltpu.CompilerParams(
            collective_id=collective, has_side_effects=True, vmem_limit_bytes=12 * 2**20
        ),
    )(*args)


def sine(index):
    angle = index * (full_turn / GRID)
    square = angle * angle
    total = jnp.full_like(square, -1.0 / 39916800.0)
    for term in (1.0 / 362880.0, -1.0 / 5040.0, 1.0 / 120.0, -1.0 / 6.0, 1.0):
        total = total * square + term
    return total * angle


def turned(index):
    index = index - GRID * jnp.floor(index * (1.0 / GRID))
    signed = index - GRID // 2
    size = jnp.abs(signed)
    near = jnp.minimum(size, GRID // 2 - size)
    return sine(size - GRID // 4), sine(jnp.where(signed < 0, near, -near))


def spline_taps(part):
    rest = 1.0 - part
    square = part * part
    cube = square * part
    weights = (
        rest * rest * rest * (1.0 / 6.0),
        (3.0 * cube - 6.0 * square + 4.0) * (1.0 / 6.0),
        (-3.0 * cube + 3.0 * square + 3.0 * part + 1.0) * (1.0 / 6.0),
        cube * (1.0 / 6.0),
    )
    slopes = (
        -0.5 * rest * rest,
        (3.0 * square - 4.0 * part) * 0.5,
        (-3.0 * square + 2.0 * part + 1.0) * 0.5,
        0.5 * square,
    )
    return weights, slopes


def mode_pairs(taps, wave):
    (cos_one, sin_one, cos_two, sin_two), (cosine, sine_part) = wave
    real = taps[1] + (taps[0] + taps[2]) * cos_one + taps[3] * cos_two
    imag = (taps[2] - taps[0]) * sin_one + taps[3] * sin_two
    return cosine * real - sine_part * imag, sine_part * real + cosine * imag


def field_kernel(
    sites_ref,
    charges_ref,
    listed_ref,
    out_ref,
    count_ref,
    packed_ref,
    wave_ref,
    high_ref,
    x_ref,
    slope_x_ref,
    y_ref,
    slope_y_ref,
    lit_ref,
    z_ref,
    slope_z_ref,
    plane_ref,
    weight_ref,
    row_ref,
    spectrum_ref,
    scaled_ref,
    found_ref,
    sem,
):
    size_x = lax.axis_size("gx")
    size_y = lax.axis_size("gy")
    columns = size_x * size_y
    modes_x = x_ref.shape[0]
    modes_y = y_ref.shape[0]
    modes_z = spectrum_ref.shape[1]
    half_x = modes_x // 2
    half_y = modes_y // 2
    half_z = modes_z // 2
    start_x = lax.axis_index("gx") * half_x
    start_y = lax.axis_index("gy") * half_y
    group = modes_x
    shape = (8, LANES)
    copy = pltpu.make_async_copy(listed_ref, count_ref, sem)
    copy.start()

    spectrum_ref[...] = jnp.zeros_like(spectrum_ref)
    found_ref[...] = jnp.zeros_like(found_ref)
    packed_ref[...] = jnp.zeros_like(packed_ref)
    sub = lax.broadcasted_iota(jnp.int32, shape, 0).astype(jnp.float32)
    lane = lax.broadcasted_iota(jnp.int32, shape, 1)
    starts = [start_x.astype(jnp.float32), start_y.astype(jnp.float32), 0.0]
    groups = [half_x // 8, half_y // 8, half_z // 8]
    firsts = [0, groups[0], groups[0] + groups[1]]
    for d in range(3):
        rows = groups[d] * 8
        mode = lax.broadcasted_iota(jnp.int32, (rows, LANES), 0).astype(jnp.float32) + starts[d]
        cosine, sine_part = turned(mode)
        double = (1.0 - 2.0 * sine_part * sine_part, 2.0 * sine_part * cosine)
        for index, value in enumerate((cosine, sine_part) + double):
            wave_ref[firsts[d] : firsts[d] + groups[d], index] = value.reshape(groups[d], 8, LANES)

    fine = LANES // 2
    spot = lax.broadcasted_iota(jnp.int32, (modes_y, modes_z), 1)
    rest = jnp.where(spot < LANES, spot, (spot - LANES) % (half_z - fine))
    mode = jnp.where(
        spot < LANES, FINE[0] * 8 + spot % fine, jnp.where(rest < FINE[0] * 8, rest, rest + fine)
    ).astype(jnp.float32)
    factor = jnp.where(mode == 0, 1.0, 2.0) * (1.0 / GRID)
    wave = mode * (full_turn / GRID)
    square = wave * wave
    spot = lax.broadcasted_iota(jnp.int32, (modes_y, modes_z), 0)
    mode = start_y + jnp.where(spot < half_y, spot, spot - half_y)
    mode = jnp.where((mode == 0) & (spot >= half_y), GRID // 2, mode)
    ends = (mode == 0) | (mode == GRID // 2)
    factor = factor * jnp.where(ends, 1.0, 2.0) * (1.0 / GRID)
    wave = mode.astype(jnp.float32) * (full_turn / GRID)
    square = square + wave * wave
    decay = -0.5 * screen_width * screen_width
    plane_ref[...] = square
    weight_ref[...] = jnp.exp(square * decay) * factor * (2.0 * full_turn)
    spot = lax.broadcasted_iota(jnp.int32, (modes_x, LANES), 0)
    mode = start_x + jnp.where(spot < half_x, spot, spot - half_x)
    mode = jnp.where((mode == 0) & (spot >= half_x), GRID // 2, mode)
    ends = (mode == 0) | (mode == GRID // 2)
    wave = mode.astype(jnp.float32) * (full_turn / GRID)
    square = wave * wave
    row_ref[0] = square
    row_ref[1] = jnp.exp(square * decay) * jnp.where(ends, 1.0, 2.0) * (1.0 / GRID)

    copy.wait()

    def pack(j, start):
        count = count_ref[j, 0]
        tile = start // LANES
        shift = start % LANES
        site = jnp.concatenate([sites_ref[j], jnp.broadcast_to(charges_ref[j], (4, LANES))], axis=0)
        turn = pltpu.roll(jnp.where(lane < count, site, 0.0), shift, 1)
        packed_ref[tile] = packed_ref[tile] + jnp.where(lane >= shift, turn, 0.0)
        packed_ref[tile + 1] = jnp.where(lane < shift, turn, 0.0)
        return start + count

    total = lax.fori_loop(0, columns, pack, 0, unroll=4)
    chunks = (total + CHUNK - 1) // CHUNK
    order = list(range(*FINE)) + list(range(FINE[0])) + list(range(FINE[1], groups[2]))

    def tables(tile, carry):
        lanes = pl.ds(pl.multiple_of(tile * LANES, LANES), LANES)
        charge = jnp.broadcast_to(packed_ref[tile, 7:8, :], shape)
        for d in range(3):
            spot = jnp.broadcast_to(packed_ref[tile, d : d + 1, :], shape)
            cell = jnp.floor(spot)
            part = spot - cell
            weights, slopes = spline_taps(part)
            low_cos, low_sin = turned(sub * cell)
            for h in range(-(-groups[d] // 8)):
                high_cos, high_sin = turned((starts[d] + 8.0 * (sub + 8.0 * h)) * cell)
                high_ref[0, 8 * h : 8 * h + 8] = high_cos
                high_ref[1, 8 * h : 8 * h + 8] = high_sin

            def pairs(g):
                high_cos = high_ref[0, g : g + 1]
                high_sin = high_ref[1, g : g + 1]
                constants = tuple(wave_ref[firsts[d] + g, index] for index in range(4))
                wave = (
                    constants,
                    (
                        high_cos * low_cos - high_sin * low_sin,
                        high_sin * low_cos + high_cos * low_sin,
                    ),
                )
                return mode_pairs(weights, wave) + mode_pairs(slopes, wave)

            if d < 2:
                half = groups[d] * 8
                for g in range(groups[d]):
                    even, odd, slope_even, slope_odd = pairs(g)
                    if g == 0:
                        parity = cell - 2.0 * jnp.floor(cell * 0.5)
                        parity = 1.0 - 2.0 * parity
                        first = (sub + starts[d]) == 0
                        last = parity * (weights[1] + weights[3] - weights[0] - weights[2])
                        odd = jnp.where(first, last, odd)
                        last = parity * (slopes[1] + slopes[3] - slopes[0] - slopes[2])
                        slope_odd = jnp.where(first, last, slope_odd)
                    table = (x_ref, y_ref)[d]
                    slope = (slope_x_ref, slope_y_ref)[d]
                    table[8 * g : 8 * g + 8, lanes] = even
                    table[half + 8 * g : half + 8 * g + 8, lanes] = odd
                    slope[8 * g : 8 * g + 8, lanes] = slope_even
                    slope[half + 8 * g : half + 8 * g + 8, lanes] = slope_odd
                    if d == 1:
                        lit_ref[8 * g : 8 * g + 8, lanes] = even * charge
                        lit_ref[half + 8 * g : half + 8 * g + 8, lanes] = odd * charge
                continue
            for index in range(0, len(order), 2):
                both = [pairs(order[index]), pairs(order[index + 1])]
                fine_part = index < FINE[1] - FINE[0]
                if fine_part:
                    spots = (8 * index, fine + 8 * index)
                else:
                    spots = (LANES + 8 * index - fine, half_z + 8 * index)
                for which in range(4):
                    table = z_ref if which < 2 else slope_z_ref
                    value = jnp.concatenate([both[0][which], both[1][which]], axis=0)
                    high = value.astype(jnp.bfloat16)
                    row = spots[which % 2]
                    table[row : row + 16, lanes] = high
                    if fine_part:
                        low = value - high.astype(jnp.float32)
                        row = row + modes_z
                        table[row : row + 16, lanes] = low.astype(jnp.bfloat16)
        return carry

    lax.fori_loop(0, chunks * (CHUNK // LANES), tables, 0)

    def gather_chunk(chunk, carry):
        lanes = pl.ds(pl.multiple_of(chunk * CHUNK, CHUNK), CHUNK)
        y = lit_ref[:, lanes]
        z = z_ref[:, lanes]

        def rows(g, inner):
            x = x_ref[pl.ds(pl.multiple_of(g * group, group), group), lanes]
            left = jnp.concatenate(
                [(x[a : a + 1] * y).astype(jnp.bfloat16) for a in range(group)], axis=0
            )
            where = pl.ds(pl.multiple_of(g * group * modes_y, group * modes_y), group * modes_y)
            form = (((1,), (1,)), ((), ()))
            both = lax.dot_general(left, z, form, preferred_element_type=jnp.float32)
            spectrum_ref[where, :LANES] += both[:, :LANES] + both[:, modes_z:]
            spectrum_ref[where, LANES:] += both[:, LANES:modes_z]
            return inner

        return lax.fori_loop(0, modes_x // group, rows, carry)

    lax.fori_loop(0, chunks, gather_chunk, 0)

    def spread(row):
        return jnp.concatenate([row] * (modes_z // LANES), axis=1)

    def apply(a, square, weight):
        green = weight / square * spread(row_ref[1, pl.ds(a, 1), :])
        where = pl.ds(pl.multiple_of(a * modes_y, modes_y), modes_y)
        value = (spectrum_ref[where, :] * green).astype(jnp.bfloat16)
        scaled_ref[where, :modes_z] = value
        scaled_ref[where, modes_z:] = value[:, :LANES]

    square = plane_ref[...] + spread(row_ref[0, 0:1, :])
    above = square > 0
    apply(0, jnp.where(above, square, 1.0), jnp.where(above, weight_ref[...], 0.0))

    def scale(a, carry):
        apply(a, plane_ref[...] + spread(row_ref[0, pl.ds(a, 1), :]), weight_ref[...])
        return carry

    lax.fori_loop(1, modes_x, scale, 0)

    def tile_step(tile, carry):
        lanes = pl.ds(pl.multiple_of(tile * TILE, TILE), TILE)
        y = y_ref[:, lanes]
        slope_y = slope_y_ref[:, lanes]
        z = z_ref[:, lanes]
        slope_z = slope_z_ref[:, lanes]

        def rows(g, sums):
            spot = pl.ds(pl.multiple_of(g * group, group), group)
            x = x_ref[spot, lanes]
            slope_x = slope_x_ref[spot, lanes]
            where = pl.ds(pl.multiple_of(g * group * modes_y, group * modes_y), group * modes_y)
            left = scaled_ref[where, :]
            along = jnp.dot(left, z, preferred_element_type=jnp.float32)
            slant = jnp.dot(left, slope_z, preferred_element_type=jnp.float32)
            value, field_x, field_y, field_z = sums
            for a in range(group):
                part = along[a * modes_y : (a + 1) * modes_y]
                skew = slant[a * modes_y : (a + 1) * modes_y]
                over = jnp.sum((part * y).reshape(modes_y // 8, 8, TILE), axis=0)
                tilt = jnp.sum((part * slope_y).reshape(modes_y // 8, 8, TILE), axis=0)
                deep = jnp.sum((skew * y).reshape(modes_y // 8, 8, TILE), axis=0)
                row = x[a : a + 1]
                value = value + over * row
                field_x = field_x + over * slope_x[a : a + 1]
                field_y = field_y + tilt * row
                field_z = field_z + deep * row
            return value, field_x, field_y, field_z

        zero = jnp.zeros((8, TILE), jnp.float32)
        sums = lax.fori_loop(0, modes_x // group, rows, (zero, zero, zero, zero))
        for part in range(TILE // LANES):
            for c in range(4):
                found_ref[tile * (TILE // LANES) + part, c : c + 1, :] = jnp.sum(
                    sums[c][:, part * LANES : (part + 1) * LANES], axis=0, keepdims=True
                )
        return carry

    lax.fori_loop(0, (total + TILE - 1) // TILE, tile_step, 0)

    def place(j, start):
        tile = start // LANES
        shift = start % LANES
        back = (LANES - shift) % LANES
        first = pltpu.roll(found_ref[tile], back, 1)
        second = pltpu.roll(found_ref[tile + 1], back, 1)
        out_ref[j] = jnp.where(lane < LANES - shift, first, second)[:4]
        return start + count_ref[j, 0]

    lax.fori_loop(0, columns, place, 0, unroll=4)


def mesh_sums(sites, charges, counts):
    size_x = lax.axis_size("gx")
    size_y = lax.axis_size("gy")
    columns, _, atoms = sites.shape
    slots = -(-(columns * atoms) // CHUNK) * CHUNK
    modes_x = GRID // size_x
    modes_y = GRID // size_y
    groups = (modes_x + modes_y + GRID) // 16
    vmem = pl.BlockSpec(memory_space=pltpu.VMEM)
    table = lambda rows: pltpu.VMEM((rows, slots), jnp.float32)
    return pl.pallas_call(
        field_kernel,
        in_specs=[vmem, vmem, vmem],
        out_specs=vmem,
        out_shape=jax.ShapeDtypeStruct((columns, 4, atoms), jnp.float32),
        scratch_shapes=[
            pltpu.SMEM(counts.shape, jnp.int32),
            pltpu.VMEM((slots // LANES + 2, 8, LANES), jnp.float32),
            pltpu.VMEM((groups, 4, 8, LANES), jnp.float32),
            pltpu.VMEM((2, 24, LANES), jnp.float32),
            table(modes_x),
            table(modes_x),
            table(modes_y),
            table(modes_y),
            table(modes_y),
            pltpu.VMEM((GRID + LANES, slots), jnp.bfloat16),
            pltpu.VMEM((GRID + LANES, slots), jnp.bfloat16),
            pltpu.VMEM((modes_y, GRID), jnp.float32),
            pltpu.VMEM((modes_y, GRID), jnp.float32),
            pltpu.VMEM((2, modes_x, LANES), jnp.float32),
            pltpu.VMEM((modes_x * modes_y, GRID), jnp.float32),
            pltpu.VMEM((modes_x * modes_y, GRID + LANES), jnp.bfloat16),
            pltpu.VMEM((slots // LANES + 2, 8, LANES), jnp.float32),
            pltpu.SemaphoreType.DMA,
        ],
        compiler_params=pltpu.CompilerParams(vmem_limit_bytes=40 * 2**20),
    )(sites, charges, counts)


def finish_kernel(sums_ref, charge_ref, energy_ref, force_ref, landed_ref, send_sem, recv_sem):
    size_y = lax.axis_size("gy")
    me = lax.axis_index("gx") * size_y + lax.axis_index("gy")
    pl.semaphore_wait(greet_peers(), lax.axis_size("gx") * size_y - 1)
    send, land = spread_piece(lambda p: sums_ref.at[p], landed_ref, send_sem, recv_sem)
    send()
    landed_ref[me] = sums_ref[me]
    land()
    total = jnp.sum(landed_ref[...], axis=0)
    charge = charge_ref[me]
    energy_ref[0] = 0.5 * charge * total[0:1]
    for c in range(3):
        force_ref[c, 0] = -charge * total[c + 1 : c + 2]


def finish(sums, charge, collective):
    peers, rows, atoms = sums.shape
    vmem = pl.BlockSpec(memory_space=pltpu.VMEM)
    return pl.pallas_call(
        finish_kernel,
        out_shape=(
            jax.ShapeDtypeStruct((1, 1, atoms), jnp.float32),
            jax.ShapeDtypeStruct((3, 1, 1, atoms), jnp.float32),
        ),
        in_specs=[vmem, vmem],
        out_specs=(vmem, vmem),
        scratch_shapes=[
            pltpu.VMEM((peers, rows, atoms), jnp.float32),
            pltpu.SemaphoreType.DMA((peers,)),
            pltpu.SemaphoreType.DMA((peers,)),
        ],
        compiler_params=pltpu.CompilerParams(
            collective_id=collective, has_side_effects=True, vmem_limit_bytes=12 * 2**20
        ),
    )(sums, charge)


def local_sites(
    positions,
    neighbours,
    live_count,
    stencil_base,
    spline_weight,
    spline_slope,
    embed_scale,
    embed_bias,
    desc_gain,
    fit_in,
    fit_bias,
    fit_hidden,
    fit_bias_two,
    fit_out,
):
    sites, charges, counts = gathered_sites(
        1,
        positions,
        neighbours,
        live_count,
        stencil_base,
        spline_slope,
        embed_scale[None, :],
        embed_bias[None, :],
        desc_gain[None, :],
        fit_in.T,
        fit_bias[None, :],
        fit_hidden,
        fit_bias_two[None, :],
        fit_out[None, :],
    )
    return finish(mesh_sums(sites, charges, counts), charges, 2)


def padded_2(shard, sides, width):
    for axis, dim in sides:
        peers, length = (lax.axis_size(axis), shard.shape[dim])
        up = [(i, (i + 1) % peers) for i in range(peers)]
        down = [(j, i) for i, j in up]
        last = lax.slice_in_dim(shard, length - width, length, axis=dim)
        leading = lax.slice_in_dim(shard, 0, width, axis=dim)
        before = lax.ppermute(last, axis, up)
        after = lax.ppermute(leading, axis, down)
        shard = jnp.concatenate([before, shard, after], axis=dim)
    return shard


def shifted(block, axis, distance):
    devices = range(lax.axis_size(axis))
    route = [((i - distance) % len(devices), i) for i in devices]
    return lax.ppermute(block, axis, route)


def stencil_table(anchor, weights, length, offset, periodic):
    count = anchor.shape[0]
    cell_index = lax.broadcasted_iota(jnp.int32, (4, length, count), 1)
    tap_index = lax.broadcasted_iota(jnp.int32, (4, length, count), 0)
    target = anchor[None, None, :] + tap_index + offset
    if periodic:
        target = target % length
    chosen = jnp.where(target == cell_index, weights[:, None, :], jnp.zeros((), weights.dtype))
    return jnp.sum(chosen, axis=0)


def spread_cells(charge, anchor, weights, extent_x, extent_y, offset, length):
    table_x = stencil_table(anchor[0], weights[0] * charge[None, :], extent_x, offset, False)
    table_y = stencil_table(anchor[1], weights[1], extent_y, offset, False)
    table_z = stencil_table(anchor[2], weights[2], length, 0, True)
    planes = (table_x[:, None, :] * table_y[None, :, :]).reshape(extent_x * extent_y, -1)
    return jnp.dot(planes, table_z.T, precision=highest).reshape(extent_x, extent_y, length)


def interpolate(padded, anchor, weights, slopes):
    extent_x, extent_y, length = padded.shape
    table_x = stencil_table(anchor[0], weights[0], extent_x, 2, False)
    slope_x = stencil_table(anchor[0], slopes[0], extent_x, 2, False)
    table_y = stencil_table(anchor[1], weights[1], extent_y, 2, False)
    slope_y = stencil_table(anchor[1], slopes[1], extent_y, 2, False)
    table_z = stencil_table(anchor[2], weights[2], length, 0, True)
    slope_z = stencil_table(anchor[2], slopes[2], length, 0, True)
    flat = padded.reshape(extent_x * extent_y, length)
    along = jnp.dot(flat, table_z, precision=highest).reshape(extent_x, extent_y, -1)
    slant = jnp.dot(flat, slope_z, precision=highest).reshape(extent_x, extent_y, -1)
    over_y = jnp.sum(along * table_y[None], axis=1)
    value = jnp.sum(table_x * over_y, axis=0)
    field_x = -jnp.sum(slope_x * over_y, axis=0)
    over_x = jnp.sum(along * table_x[:, None, :], axis=0)
    field_y = -jnp.sum(slope_y * over_x, axis=0)
    slant_y = jnp.sum(slant * table_y[None], axis=1)
    field_z = -jnp.sum(table_x * slant_y, axis=0)
    return (value, jnp.stack([field_x, field_y, field_z]))


def fitted_charge(
    nearby,
    listed,
    count,
    embed_scale,
    embed_bias,
    desc_gain,
    fit_in,
    fit_bias,
    fit_hidden,
    fit_bias_two,
    fit_out,
):
    atoms = listed.shape[1]
    center = nearby[:, 4 * atoms : 5 * atoms]
    picked = jnp.take(nearby, listed.reshape(-1), axis=1).reshape(3, listed.shape[0], atoms)
    delta = picked - center[:, None, :]
    radius = jnp.sqrt(jnp.sum(delta * delta, axis=0))
    smooth = 1.0 / (1.0 + radius / radius_scale)
    factor = smooth / (radius + radius_scale)
    envelope = jnp.concatenate([smooth[None], delta * factor[None]], axis=0)
    embed = jnp.tanh(smooth[None] * embed_scale[:, None, None] + embed_bias[:, None, None])
    mixed = jnp.einsum("ekn,ckn->ecn", embed, envelope, precision=highest)
    descriptor = jnp.einsum("ecn,acn->ean", mixed, mixed[:AXIS], precision=highest).reshape(
        -1, atoms
    )
    scaling = lax.rsqrt(jnp.mean(descriptor * descriptor, axis=0) + norm_floor)
    normed = (descriptor * scaling[None, :] * desc_gain[:, None]).astype(jnp.bfloat16)
    first = jnp.tanh(
        jnp.dot(fit_in, normed, preferred_element_type=jnp.float32) + fit_bias[:, None]
    )
    second = (
        jnp.tanh(
            jnp.dot(fit_hidden, first.astype(jnp.bfloat16), preferred_element_type=jnp.float32)
            + fit_bias_two[:, None]
        )
        + first
    )
    charge = jnp.sum(fit_out[:, None] * second, axis=0)
    slot_index = lax.broadcasted_iota(jnp.int32, (atoms,), 0)
    return jnp.where(slot_index < count, charge, jnp.zeros((), charge.dtype))


def wave_number(index, length):
    signed = jnp.where(index > length // 2, index - length, index)
    return signed.astype(jnp.float32) * (full_turn / length)


def green_values(index_x, index_y, index_z, length):
    wave_x = wave_number(index_x, length)
    wave_y = wave_number(index_y, length)
    wave_z = wave_number(index_z, length)
    square = wave_x * wave_x + wave_y * wave_y + wave_z * wave_z
    safe = jnp.where(square > 0, square, 1.0)
    value = 2.0 * full_turn * jnp.exp(-0.5 * screen_width * screen_width * square) / safe
    keep = (square > 0) & (index_z != length // 2)
    return jnp.where(keep, value, 0.0)


def wave_tables(length, count):
    rows = lax.broadcasted_iota(jnp.int32, (length, count), 0)
    cols = lax.broadcasted_iota(jnp.int32, (length, count), 1)
    angle = (rows * cols % length).astype(jnp.float32) * (full_turn / length)
    return (jnp.cos(angle), jnp.sin(angle))


def along_axis(real_part, imag_part, cosine, sine, sign, form):
    real_cos = jnp.einsum(form, real_part, cosine, precision=highest)
    real_sin = jnp.einsum(form, real_part, sine, precision=highest)
    imag_cos = jnp.einsum(form, imag_part, cosine, precision=highest)
    imag_sin = jnp.einsum(form, imag_part, sine, precision=highest)
    return (real_cos + sign * imag_sin, imag_cos - sign * real_sin)


def local_mesh(
    positions,
    neighbours,
    live_count,
    stencil_base,
    spline_weight,
    spline_slope,
    embed_scale,
    embed_bias,
    desc_gain,
    fit_in,
    fit_bias,
    fit_hidden,
    fit_bias_two,
    fit_out,
):
    columns_y = lax.axis_size("gy")
    width_x = GRID // lax.axis_size("gx")
    width_y = GRID // columns_y
    atoms = positions.shape[3]
    beside_all = padded_2(positions, (("gx", 1), ("gy", 2)), 1)
    block_x = lax.broadcasted_iota(jnp.int32, (3, 3, atoms), 0) - 1
    block_y = lax.broadcasted_iota(jnp.int32, (3, 3, atoms), 1) - 1
    offsets = jnp.stack([block_x * width_x, block_y * width_y, jnp.zeros_like(block_x)]).astype(
        jnp.float32
    )
    nearby = (beside_all + offsets).reshape(3, 9 * atoms)
    charge = fitted_charge(
        nearby,
        neighbours[:, 0, 0, :],
        live_count[0, 0],
        embed_scale,
        embed_bias,
        desc_gain,
        fit_in,
        fit_bias,
        fit_hidden,
        fit_bias_two,
        fit_out,
    )
    anchor = stencil_base[:, 0, 0, :]
    weights = spline_weight[:, :, 0, 0, :]
    slopes = spline_slope[:, :, 0, 0, :]
    spread = spread_cells(charge, anchor, weights, width_x + 4, width_y + 4, 2, GRID)
    inner = spread[2 : width_x + 2]
    for stride in (1, -1):
        piece = spread[width_x + 2 :] if stride == 1 else spread[:2]
        moved = shifted(piece, "gx", stride)
        if stride == 1:
            inner = inner.at[:2].add(moved)
        else:
            inner = inner.at[width_x - 2 :].add(moved)
    density = inner[:, 2 : width_y + 2]
    for stride in (1, -1):
        piece = inner[:, width_y + 2 :] if stride == 1 else inner[:, :2]
        moved = shifted(piece, "gy", stride)
        if stride == 1:
            density = density.at[:, :2].add(moved)
        else:
            density = density.at[:, width_y - 2 :].add(moved)
    freqs = GRID // 2
    fold_weight = jnp.where(jnp.arange(freqs) == 0, 1.0, 2.0).astype(jnp.float32) / GRID
    cosine_z, sine_z = wave_tables(GRID, freqs)
    flat = density.reshape(width_x * width_y, GRID)
    real_part = jnp.dot(flat, cosine_z, precision=highest).reshape(width_x, width_y, freqs)
    imag_part = -jnp.dot(flat, sine_z, precision=highest).reshape(width_x, width_y, freqs)
    real_part, imag_part = (
        lax.all_to_all(real_part, "gy", split_axis=2, concat_axis=1, tiled=True),
        lax.all_to_all(imag_part, "gy", split_axis=2, concat_axis=1, tiled=True),
    )
    cosine, sine = wave_tables(GRID, GRID)
    real_part, imag_part = along_axis(real_part, imag_part, cosine, sine, 1.0, "xym,yk->xkm")
    real_part, imag_part = (
        lax.all_to_all(real_part, "gx", split_axis=1, concat_axis=0, tiled=True),
        lax.all_to_all(imag_part, "gx", split_axis=1, concat_axis=0, tiled=True),
    )
    real_part, imag_part = along_axis(real_part, imag_part, cosine, sine, 1.0, "xym,xk->kym")
    span_y = real_part.shape[1]
    span_z = real_part.shape[2]
    index_x = lax.broadcasted_iota(jnp.int32, (GRID, span_y, span_z), 0)
    index_y = lax.axis_index("gx") * span_y + lax.broadcasted_iota(
        jnp.int32, (GRID, span_y, span_z), 1
    )
    index_z = lax.axis_index("gy") * span_z + lax.broadcasted_iota(
        jnp.int32, (GRID, span_y, span_z), 2
    )
    green = green_values(index_x, index_y, index_z, GRID)
    real_part = real_part * green
    imag_part = imag_part * green
    back_cos = cosine / GRID
    back_sin = sine / GRID
    real_part, imag_part = along_axis(real_part, imag_part, back_cos, back_sin, -1.0, "xym,xk->kym")
    real_part, imag_part = (
        lax.all_to_all(real_part, "gx", split_axis=0, concat_axis=1, tiled=True),
        lax.all_to_all(imag_part, "gx", split_axis=0, concat_axis=1, tiled=True),
    )
    real_part, imag_part = along_axis(real_part, imag_part, back_cos, back_sin, -1.0, "xym,yk->xkm")
    real_part, imag_part = (
        lax.all_to_all(real_part, "gy", split_axis=1, concat_axis=2, tiled=True),
        lax.all_to_all(imag_part, "gy", split_axis=1, concat_axis=2, tiled=True),
    )
    rows_y = real_part.shape[1]
    flat_real = real_part.reshape(width_x * rows_y, freqs)
    flat_imag = imag_part.reshape(width_x * rows_y, freqs)
    summed_cos = (cosine_z * fold_weight[None, :]).T
    summed_sin = (sine_z * fold_weight[None, :]).T
    potential = jnp.dot(flat_real, summed_cos, precision=highest) - jnp.dot(
        flat_imag, summed_sin, precision=highest
    )
    potential = potential.reshape(width_x, rows_y, GRID)
    padded = padded_2(potential, (("gx", 0), ("gy", 1)), 2)
    value, field = interpolate(padded, anchor, weights, slopes)
    energy = (0.5 * charge * value).reshape(1, 1, atoms)
    force = (charge[None, :] * field).reshape(3, 1, 1, atoms)
    return (energy, force)


def solution(mesh):
    def local(positions, *rest):
        columns_x, columns_y = (lax.axis_size("gx"), lax.axis_size("gy"))
        sites = columns_x * columns_y * positions.shape[3]
        whole = GRID % (16 * columns_x) == 0 and GRID % (16 * columns_y) == 0
        few = whole and sites <= 8 * GRID * 2
        return (local_sites if few and positions.shape[3] == LANES else local_mesh)(positions, *rest)

    placed = (
        P(None, "gx", "gy", None),
        P(None, "gx", "gy", None),
        P("gx", "gy"),
        P(None, "gx", "gy", None),
        P(None, None, "gx", "gy", None),
        P(None, None, "gx", "gy", None),
        P(),
        P(),
        P(),
        P(),
        P(),
        P(),
        P(),
        P(),
    )
    return jax.shard_map(
        local,
        mesh=mesh,
        in_specs=placed,
        out_specs=(P("gx", "gy", None), P(None, "gx", "gy", None)),
        check_vma=False,
    )
```

```python
import math

import jax
import jax.numpy as jnp
from jax import lax
from jax.experimental import pallas as pl
from jax.experimental.pallas import tpu as pltpu
from jax.sharding import PartitionSpec as P

GRID = 384
AXIS = 16
LANES = 128
CHUNK = 256
TILE = 256
FINE = (5, 13)

highest = lax.Precision.HIGHEST
radius_scale = 4.0
screen_width = 0.25
norm_floor = 1e-06
full_turn = 2.0 * math.pi


def each_peer(visit):
    size_x = lax.axis_size("gx")
    size_y = lax.axis_size("gy")
    place_x = lax.axis_index("gx")
    place_y = lax.axis_index("gy")
    across = [(place_y + b) % size_y for b in range(size_y)]
    for b in range(1, size_y):
        visit(b, place_x, across[b])

    def row(a, carry):
        x = (place_x + a) % size_x
        for b in range(size_y):
            visit(a * size_y + b, x, across[b])
        return carry

    lax.fori_loop(1, size_x, row, 0)


def greet_peers():
    barrier = pltpu.get_barrier_semaphore()

    def greet(k, x, y):
        pl.semaphore_signal(
            barrier, inc=1, device_id=(x, y), device_id_type=pl.DeviceIdType.MESH
        )

    each_peer(greet)
    return barrier


def spread_piece(piece, whole_ref, send_sem, recv_sem):
    size_y = lax.axis_size("gy")
    peers = lax.axis_size("gx") * size_y
    me = lax.axis_index("gx") * size_y + lax.axis_index("gy")

    def send(k, x, y):
        pltpu.make_async_remote_copy(
            src_ref=piece(x * size_y + y),
            dst_ref=whole_ref.at[me],
            send_sem=send_sem,
            recv_sem=recv_sem,
            device_id=(x, y),
            device_id_type=pl.DeviceIdType.MESH,
        ).start()

    def land():
        others = whole_ref.at[pl.ds(0, peers - 1)]
        pltpu.make_async_copy(others, others, send_sem).wait()
        pltpu.make_async_copy(others, others, recv_sem).wait()

    return (lambda: each_peer(send)), land


def column(table, index, length):
    return jnp.broadcast_to(table[:length, index : index + 1], (length, LANES))


def site_kernel(
    position_ref,
    neighbour_ref,
    count_ref,
    base_ref,
    slope_ref,
    scale_ref,
    bias_ref,
    gain_ref,
    fit_in_hbm,
    fit_bias_ref,
    fit_hidden_hbm,
    fit_bias_two_ref,
    fit_out_ref,
    sites_ref,
    charges_ref,
    counts_ref,
    place_ref,
    parcel_ref,
    own_ref,
    near_ref,
    listed_ref,
    rows_ref,
    columns_ref,
    gains_ref,
    env_ref,
    mixed_ref,
    descriptor_ref,
    normed_ref,
    fit_in_ref,
    fit_hidden_ref,
    load_sem,
    near_send,
    near_recv,
    site_send,
    site_recv,
    charge_send,
    charge_recv,
):
    size_x = lax.axis_size("gx")
    size_y = lax.axis_size("gy")
    peers = size_x * size_y
    place_x = lax.axis_index("gx")
    place_y = lax.axis_index("gy")
    me = place_x * size_y + place_y
    width_x = GRID // size_x
    width_y = GRID // size_y
    neigh = neighbour_ref.shape[0]
    atoms = neighbour_ref.shape[3]
    width = scale_ref.shape[1]
    features = gain_ref.shape[1]
    loads = [
        pltpu.make_async_copy(fit_in_hbm, fit_in_ref, load_sem.at[0]),
        pltpu.make_async_copy(fit_hidden_hbm, fit_hidden_ref, load_sem.at[1]),
    ]
    for load in loads:
        load.start()
    barrier = greet_peers()

    count = count_ref[0, 0]
    origin = (place_x * width_x + 1, place_y * width_y + 1, 1)
    place_ref[...] = jnp.zeros_like(place_ref)
    for c in range(3):
        place_ref[c : c + 1, :] = position_ref[c, 0]
        part = slope_ref[c, 0, 0] + slope_ref[c, 3, 0] + 0.5
        parcel_ref[c : c + 1, :] = (base_ref[c, 0] + origin[c]).astype(jnp.float32) + part
    parcel_ref[3:4, :] = jnp.full((1, atoms), count, jnp.int32).astype(jnp.float32)
    for k in range(neigh):
        listed_ref[k : k + 1, :] = neighbour_ref[k, 0]

    pl.semaphore_wait(barrier, peers - 1)

    def near_copy(slot, target):
        return pltpu.make_async_remote_copy(
            src_ref=place_ref,
            dst_ref=near_ref.at[slot],
            send_sem=near_send.at[slot],
            recv_sem=near_recv.at[slot],
            device_id=target,
            device_id_type=pl.DeviceIdType.MESH,
        )

    around = [(a, b) for a in (-1, 0, 1) for b in (-1, 0, 1)]
    targets = [((place_x - a) % size_x, (place_y - b) % size_y) for a, b in around]
    for slot in range(9):
        if slot != 4:
            near_copy(slot, targets[slot]).start()

    send_sites, land_sites = spread_piece(lambda p: parcel_ref, sites_ref, site_send, site_recv)
    send_sites()
    near_ref[4] = place_ref[...]
    sites_ref[me] = parcel_ref[...]

    rows_ref[...] = jnp.zeros_like(rows_ref)
    for index, ref in enumerate((scale_ref, bias_ref)):
        rows_ref[index : index + 1, :width] = ref[...]
    for index, ref in enumerate((fit_bias_ref, fit_bias_two_ref, fit_out_ref)):
        rows_ref[index + 2 : index + 3, :] = ref[...]
    parts = -(-features // LANES)
    for part in range(parts):
        size = min(LANES, features - part * LANES)
        rows_ref[part + 5 : part + 6, :size] = gain_ref[:, part * LANES : part * LANES + size]
    columns_ref[...] = rows_ref[...].T
    for part in range(parts):
        size = min(LANES, features - part * LANES)
        gains_ref[part * LANES : part * LANES + size, :] = column(columns_ref, part + 5, size)

    for slot in range(9):
        if slot != 4:
            near_copy(slot, targets[slot]).wait_send()
            near_copy(slot, targets[slot]).wait_recv()

    listed = listed_ref[...]
    slots = listed % atoms
    blocks = listed // atoms
    square = jnp.zeros((neigh, atoms), jnp.float32)
    deltas = []
    for c in range(3):
        center = near_ref[4, c : c + 1, :]
        picked = jnp.zeros((neigh, atoms), jnp.float32)
        for slot, (a, b) in enumerate(around):
            offset = (a * width_x, b * width_y, 0)[c]
            row = jnp.broadcast_to(near_ref[slot, c : c + 1, :] + float(offset), (neigh, atoms))
            got = jnp.take_along_axis(row, slots, axis=1, mode="promise_in_bounds")
            picked = jnp.where(blocks == slot, got, picked)
        delta = picked - center
        deltas.append(delta)
        square = square + delta * delta
    radius = jnp.sqrt(square)
    smooth = 1.0 / (1.0 + radius / radius_scale)
    factor = smooth / (radius + radius_scale)
    env_ref[0] = smooth
    for c in range(3):
        env_ref[c + 1] = deltas[c] * factor

    padded = mixed_ref.shape[1]
    bounds = [(0, padded // 16 * 8), (padded // 16 * 8, padded)]
    for first, last in bounds:
        span = last - first
        scale = jnp.broadcast_to(columns_ref[first:last, 0:1], (span, atoms))
        shift = jnp.broadcast_to(columns_ref[first:last, 1:2], (span, atoms))

        def step(k, sums):
            rows = [env_ref[c, pl.ds(k, 1), :] for c in range(4)]
            embed = jnp.tanh(rows[0] * scale + shift)
            return tuple(total + embed * row for total, row in zip(sums, rows))

        zero = jnp.zeros((span, atoms), jnp.float32)
        sums = lax.fori_loop(0, neigh, step, (zero, zero, zero, zero), unroll=2)
        for c in range(4):
            mixed_ref[c, first:last, :] = sums[c]

    def describe(e, total):
        value = jnp.zeros((AXIS, atoms), jnp.float32)
        for c in range(4):
            value = value + mixed_ref[c, pl.ds(e, 1), :] * mixed_ref[c, :AXIS, :]
        descriptor_ref[pl.ds(pl.multiple_of(e * AXIS, AXIS), AXIS), :] = value
        return total + value * value

    total = lax.fori_loop(0, width, describe, jnp.zeros((AXIS, atoms), jnp.float32), unroll=4)
    mean = jnp.sum(total, axis=0, keepdims=True) / features
    scaling = lax.rsqrt(mean + norm_floor)
    normed_ref[...] = (descriptor_ref[...] * scaling * gains_ref[...]).astype(jnp.bfloat16)
    for load in loads:
        load.wait()
    first = lax.dot_general(
        fit_in_ref[...],
        normed_ref[...],
        (((0,), (0,)), ((), ())),
        preferred_element_type=jnp.float32,
    )
    first = jnp.tanh(first + column(columns_ref, 2, LANES))
    second = jnp.dot(
        fit_hidden_ref[...], first.astype(jnp.bfloat16), preferred_element_type=jnp.float32
    )
    second = jnp.tanh(second + column(columns_ref, 3, LANES)) + first
    charge = jnp.sum(column(columns_ref, 4, LANES) * second, axis=0, keepdims=True)
    lane = lax.broadcasted_iota(jnp.int32, (1, atoms), 1)
    own_ref[...] = jnp.where(lane < count, charge, 0.0)

    send_charges, land_charges = spread_piece(
        lambda p: own_ref, charges_ref, charge_send, charge_recv
    )
    send_charges()
    charges_ref[me] = own_ref[...]
    land_sites()
    for p in range(peers):
        counts_ref[p : p + 1, :] = sites_ref[p, 3:4, :].astype(jnp.int32)
    land_charges()


def gathered_sites(collective, *args):
    peers = lax.axis_size("gx") * lax.axis_size("gy")
    neigh = args[1].shape[0]
    atoms = args[1].shape[3]
    width = args[5].shape[1]
    features = args[7].shape[1]
    padded = -(-width // 8) * 8
    vmem = pl.BlockSpec(memory_space=pltpu.VMEM)
    smem = pl.BlockSpec(memory_space=pltpu.SMEM)
    hbm = pl.BlockSpec(memory_space=pltpu.HBM)
    dma = pltpu.SemaphoreType.DMA
    return pl.pallas_call(
        site_kernel,
        in_specs=[vmem, vmem, smem] + [vmem] * 5 + [hbm, vmem, hbm, vmem, vmem],
        out_specs=(vmem, vmem, vmem),
        out_shape=(
            jax.ShapeDtypeStruct((peers, 4, atoms), jnp.float32),
            jax.ShapeDtypeStruct((peers, 1, atoms), jnp.float32),
            jax.ShapeDtypeStruct((peers, atoms), jnp.int32),
        ),
        scratch_shapes=[
            pltpu.VMEM((4, atoms), jnp.float32),
            pltpu.VMEM((4, atoms), jnp.float32),
            pltpu.VMEM((1, atoms), jnp.float32),
            pltpu.VMEM((9, 4, atoms), jnp.float32),
            pltpu.VMEM((neigh, atoms), jnp.int32),
            pltpu.VMEM((LANES, LANES), jnp.float32),
            pltpu.VMEM((LANES, LANES), jnp.float32),
            pltpu.VMEM((features, atoms), jnp.float32),
            pltpu.VMEM((4, neigh, atoms), jnp.float32),
            pltpu.VMEM((4, padded, atoms), jnp.float32),
            pltpu.VMEM((features, atoms), jnp.float32),
            pltpu.VMEM((features, atoms), jnp.bfloat16),
            pltpu.VMEM(args[8].shape, args[8].dtype),
            pltpu.VMEM(args[10].shape, args[10].dtype),
            dma((2,)),
            dma((9,)),
            dma((9,)),
            dma,
            dma,
            dma,
            dma,
        ],
        compiler_params=pltpu.CompilerParams(
            collective_id=collective, has_side_effects=True, vmem_limit_bytes=12 * 2**20
        ),
    )(*args)


def sine(index):
    angle = index * (full_turn / GRID)
    square = angle * angle
    total = jnp.full_like(square, -1.0 / 39916800.0)
    for term in (1.0 / 362880.0, -1.0 / 5040.0, 1.0 / 120.0, -1.0 / 6.0, 1.0):
        total = total * square + term
    return total * angle


def turned(index):
    index = index - GRID * jnp.floor(index * (1.0 / GRID))
    signed = index - GRID // 2
    size = jnp.abs(signed)
    near = jnp.minimum(size, GRID // 2 - size)
    return sine(size - GRID // 4), sine(jnp.where(signed < 0, near, -near))


def spline_taps(part):
    rest = 1.0 - part
    square = part * part
    cube = square * part
    weights = (
        rest * rest * rest * (1.0 / 6.0),
        (3.0 * cube - 6.0 * square + 4.0) * (1.0 / 6.0),
        (-3.0 * cube + 3.0 * square + 3.0 * part + 1.0) * (1.0 / 6.0),
        cube * (1.0 / 6.0),
    )
    slopes = (
        -0.5 * rest * rest,
        (3.0 * square - 4.0 * part) * 0.5,
        (-3.0 * square + 2.0 * part + 1.0) * 0.5,
        0.5 * square,
    )
    return weights, slopes


def mode_pairs(taps, wave):
    (cos_one, sin_one, cos_two, sin_two), (cosine, sine_part) = wave
    real = taps[1] + (taps[0] + taps[2]) * cos_one + taps[3] * cos_two
    imag = (taps[2] - taps[0]) * sin_one + taps[3] * sin_two
    return cosine * real - sine_part * imag, sine_part * real + cosine * imag


def field_kernel(
    sites_ref,
    charges_ref,
    listed_ref,
    out_ref,
    count_ref,
    packed_ref,
    wave_ref,
    high_ref,
    x_ref,
    slope_x_ref,
    y_ref,
    slope_y_ref,
    lit_ref,
    z_ref,
    slope_z_ref,
    plane_ref,
    weight_ref,
    row_ref,
    spectrum_ref,
    scaled_ref,
    found_ref,
    sem,
):
    size_x = lax.axis_size("gx")
    size_y = lax.axis_size("gy")
    columns = size_x * size_y
    modes_x = x_ref.shape[0]
    modes_y = y_ref.shape[0]
    modes_z = spectrum_ref.shape[1]
    half_x = modes_x // 2
    half_y = modes_y // 2
    half_z = modes_z // 2
    start_x = lax.axis_index("gx") * half_x
    start_y = lax.axis_index("gy") * half_y
    group = modes_x
    shape = (8, LANES)
    copy = pltpu.make_async_copy(listed_ref, count_ref, sem)
    copy.start()

    spectrum_ref[...] = jnp.zeros_like(spectrum_ref)
    found_ref[...] = jnp.zeros_like(found_ref)
    packed_ref[...] = jnp.zeros_like(packed_ref)
    sub = lax.broadcasted_iota(jnp.int32, shape, 0).astype(jnp.float32)
    lane = lax.broadcasted_iota(jnp.int32, shape, 1)
    starts = [start_x.astype(jnp.float32), start_y.astype(jnp.float32), 0.0]
    groups = [half_x // 8, half_y // 8, half_z // 8]
    firsts = [0, groups[0], groups[0] + groups[1]]
    for d in range(3):
        rows = groups[d] * 8
        mode = lax.broadcasted_iota(jnp.int32, (rows, LANES), 0).astype(jnp.float32) + starts[d]
        cosine, sine_part = turned(mode)
        double = (1.0 - 2.0 * sine_part * sine_part, 2.0 * sine_part * cosine)
        for index, value in enumerate((cosine, sine_part) + double):
            wave_ref[firsts[d] : firsts[d] + groups[d], index] = value.reshape(groups[d], 8, LANES)

    fine = LANES // 2
    spot = lax.broadcasted_iota(jnp.int32, (modes_y, modes_z), 1)
    rest = jnp.where(spot < LANES, spot, (spot - LANES) % (half_z - fine))
    mode = jnp.where(
        spot < LANES, FINE[0] * 8 + spot % fine, jnp.where(rest < FINE[0] * 8, rest, rest + fine)
    ).astype(jnp.float32)
    factor = jnp.where(mode == 0, 1.0, 2.0) * (1.0 / GRID)
    wave = mode * (full_turn / GRID)
    square = wave * wave
    spot = lax.broadcasted_iota(jnp.int32, (modes_y, modes_z), 0)
    mode = start_y + jnp.where(spot < half_y, spot, spot - half_y)
    mode = jnp.where((mode == 0) & (spot >= half_y), GRID // 2, mode)
    ends = (mode == 0) | (mode == GRID // 2)
    factor = factor * jnp.where(ends, 1.0, 2.0) * (1.0 / GRID)
    wave = mode.astype(jnp.float32) * (full_turn / GRID)
    square = square + wave * wave
    decay = -0.5 * screen_width * screen_width
    plane_ref[...] = square
    weight_ref[...] = jnp.exp(square * decay) * factor * (2.0 * full_turn)
    spot = lax.broadcasted_iota(jnp.int32, (modes_x, LANES), 0)
    mode = start_x + jnp.where(spot < half_x, spot, spot - half_x)
    mode = jnp.where((mode == 0) & (spot >= half_x), GRID // 2, mode)
    ends = (mode == 0) | (mode == GRID // 2)
    wave = mode.astype(jnp.float32) * (full_turn / GRID)
    square = wave * wave
    row_ref[0] = square
    row_ref[1] = jnp.exp(square * decay) * jnp.where(ends, 1.0, 2.0) * (1.0 / GRID)

    copy.wait()

    def pack(j, start):
        count = count_ref[j, 0]
        tile = start // LANES
        shift = start % LANES
        site = jnp.concatenate([sites_ref[j], jnp.broadcast_to(charges_ref[j], (4, LANES))], axis=0)
        turn = pltpu.roll(jnp.where(lane < count, site, 0.0), shift, 1)
        packed_ref[tile] = packed_ref[tile] + jnp.where(lane >= shift, turn, 0.0)
        packed_ref[tile + 1] = jnp.where(lane < shift, turn, 0.0)
        return start + count

    total = lax.fori_loop(0, columns, pack, 0, unroll=4)
    chunks = (total + CHUNK - 1) // CHUNK
    order = list(range(*FINE)) + list(range(FINE[0])) + list(range(FINE[1], groups[2]))

    def tables(tile, carry):
        lanes = pl.ds(pl.multiple_of(tile * LANES, LANES), LANES)
        charge = jnp.broadcast_to(packed_ref[tile, 7:8, :], shape)
        for d in range(3):
            spot = jnp.broadcast_to(packed_ref[tile, d : d + 1, :], shape)
            cell = jnp.floor(spot)
            part = spot - cell
            weights, slopes = spline_taps(part)
            low_cos, low_sin = turned(sub * cell)
            for h in range(-(-groups[d] // 8)):
                high_cos, high_sin = turned((starts[d] + 8.0 * (sub + 8.0 * h)) * cell)
                high_ref[0, 8 * h : 8 * h + 8] = high_cos
                high_ref[1, 8 * h : 8 * h + 8] = high_sin

            def pairs(g):
                high_cos = high_ref[0, g : g + 1]
                high_sin = high_ref[1, g : g + 1]
                constants = tuple(wave_ref[firsts[d] + g, index] for index in range(4))
                wave = (
                    constants,
                    (
                        high_cos * low_cos - high_sin * low_sin,
                        high_sin * low_cos + high_cos * low_sin,
                    ),
                )
                return mode_pairs(weights, wave) + mode_pairs(slopes, wave)

            if d < 2:
                half = groups[d] * 8
                for g in range(groups[d]):
                    even, odd, slope_even, slope_odd = pairs(g)
                    if g == 0:
                        parity = cell - 2.0 * jnp.floor(cell * 0.5)
                        parity = 1.0 - 2.0 * parity
                        first = (sub + starts[d]) == 0
                        last = parity * (weights[1] + weights[3] - weights[0] - weights[2])
                        odd = jnp.where(first, last, odd)
                        last = parity * (slopes[1] + slopes[3] - slopes[0] - slopes[2])
                        slope_odd = jnp.where(first, last, slope_odd)
                    table = (x_ref, y_ref)[d]
                    slope = (slope_x_ref, slope_y_ref)[d]
                    table[8 * g : 8 * g + 8, lanes] = even
                    table[half + 8 * g : half + 8 * g + 8, lanes] = odd
                    slope[8 * g : 8 * g + 8, lanes] = slope_even
                    slope[half + 8 * g : half + 8 * g + 8, lanes] = slope_odd
                    if d == 1:
                        lit_ref[8 * g : 8 * g + 8, lanes] = even * charge
                        lit_ref[half + 8 * g : half + 8 * g + 8, lanes] = odd * charge
                continue
            for index in range(0, len(order), 2):
                both = [pairs(order[index]), pairs(order[index + 1])]
                fine_part = index < FINE[1] - FINE[0]
                if fine_part:
                    spots = (8 * index, fine + 8 * index)
                else:
                    spots = (LANES + 8 * index - fine, half_z + 8 * index)
                for which in range(4):
                    table = z_ref if which < 2 else slope_z_ref
                    value = jnp.concatenate([both[0][which], both[1][which]], axis=0)
                    high = value.astype(jnp.bfloat16)
                    row = spots[which % 2]
                    table[row : row + 16, lanes] = high
                    if fine_part:
                        low = value - high.astype(jnp.float32)
                        row = row + modes_z
                        table[row : row + 16, lanes] = low.astype(jnp.bfloat16)
        return carry

    lax.fori_loop(0, chunks * (CHUNK // LANES), tables, 0)

    def gather_chunk(chunk, carry):
        lanes = pl.ds(pl.multiple_of(chunk * CHUNK, CHUNK), CHUNK)
        y = lit_ref[:, lanes]
        z = z_ref[:, lanes]

        def rows(g, inner):
            x = x_ref[pl.ds(pl.multiple_of(g * group, group), group), lanes]
            left = jnp.concatenate(
                [(x[a : a + 1] * y).astype(jnp.bfloat16) for a in range(group)], axis=0
            )
            where = pl.ds(pl.multiple_of(g * group * modes_y, group * modes_y), group * modes_y)
            form = (((1,), (1,)), ((), ()))
            both = lax.dot_general(left, z, form, preferred_element_type=jnp.float32)
            spectrum_ref[where, :LANES] += both[:, :LANES] + both[:, modes_z:]
            spectrum_ref[where, LANES:] += both[:, LANES:modes_z]
            return inner

        return lax.fori_loop(0, modes_x // group, rows, carry)

    lax.fori_loop(0, chunks, gather_chunk, 0)

    def spread(row):
        return jnp.concatenate([row] * (modes_z // LANES), axis=1)

    def apply(a, square, weight):
        green = weight / square * spread(row_ref[1, pl.ds(a, 1), :])
        where = pl.ds(pl.multiple_of(a * modes_y, modes_y), modes_y)
        value = (spectrum_ref[where, :] * green).astype(jnp.bfloat16)
        scaled_ref[where, :modes_z] = value
        scaled_ref[where, modes_z:] = value[:, :LANES]

    square = plane_ref[...] + spread(row_ref[0, 0:1, :])
    above = square > 0
    apply(0, jnp.where(above, square, 1.0), jnp.where(above, weight_ref[...], 0.0))

    def scale(a, carry):
        apply(a, plane_ref[...] + spread(row_ref[0, pl.ds(a, 1), :]), weight_ref[...])
        return carry

    lax.fori_loop(1, modes_x, scale, 0, unroll=2)

    def site_sums(block, width):
        lanes = pl.ds(pl.multiple_of(block * LANES, width), width)
        y = y_ref[:, lanes]
        slope_y = slope_y_ref[:, lanes]
        x = x_ref[:, lanes]
        slope_x = slope_x_ref[:, lanes]
        paired = jnp.concatenate([z_ref[:, lanes], slope_z_ref[:, lanes]], axis=1)
        both = jnp.dot(scaled_ref[...], paired, preferred_element_type=jnp.float32)
        value = field_x = field_y = field_z = jnp.zeros((8, width), jnp.float32)
        for a in range(modes_x):
            part = both[a * modes_y : (a + 1) * modes_y, :width]
            skew = both[a * modes_y : (a + 1) * modes_y, width:]
            over = jnp.sum((part * y).reshape(modes_y // 8, 8, width), axis=0)
            tilt = jnp.sum((part * slope_y).reshape(modes_y // 8, 8, width), axis=0)
            deep = jnp.sum((skew * y).reshape(modes_y // 8, 8, width), axis=0)
            row = x[a : a + 1]
            value = value + over * row
            field_x = field_x + over * slope_x[a : a + 1]
            field_y = field_y + tilt * row
            field_z = field_z + deep * row
        for part in range(width // LANES):
            for c, found in enumerate((value, field_x, field_y, field_z)):
                found_ref[block + part, c : c + 1, :] = jnp.sum(
                    found[:, part * LANES : (part + 1) * LANES], axis=0, keepdims=True
                )

    def tile_step(tile, carry):
        site_sums(tile * (TILE // LANES), TILE)
        return carry

    blocks = (total + LANES - 1) // LANES
    pairs_of = blocks // (TILE // LANES)
    lax.fori_loop(0, pairs_of, tile_step, 0)

    @pl.when(blocks % (TILE // LANES) > 0)
    def _():
        site_sums(pairs_of * (TILE // LANES), LANES)

    def place(j, start):
        tile = start // LANES
        shift = start % LANES
        back = (LANES - shift) % LANES
        first = pltpu.roll(found_ref[tile], back, 1)
        second = pltpu.roll(found_ref[tile + 1], back, 1)
        out_ref[j] = jnp.where(lane < LANES - shift, first, second)[:4]
        return start + count_ref[j, 0]

    lax.fori_loop(0, columns, place, 0, unroll=4)


def mesh_sums(sites, charges, counts):
    size_x = lax.axis_size("gx")
    size_y = lax.axis_size("gy")
    columns, _, atoms = sites.shape
    slots = -(-(columns * atoms) // CHUNK) * CHUNK
    modes_x = GRID // size_x
    modes_y = GRID // size_y
    groups = (modes_x + modes_y + GRID) // 16
    vmem = pl.BlockSpec(memory_space=pltpu.VMEM)
    table = lambda rows: pltpu.VMEM((rows, slots), jnp.float32)
    return pl.pallas_call(
        field_kernel,
        in_specs=[vmem, vmem, vmem],
        out_specs=vmem,
        out_shape=jax.ShapeDtypeStruct((columns, 4, atoms), jnp.float32),
        scratch_shapes=[
            pltpu.SMEM(counts.shape, jnp.int32),
            pltpu.VMEM((slots // LANES + 2, 8, LANES), jnp.float32),
            pltpu.VMEM((groups, 4, 8, LANES), jnp.float32),
            pltpu.VMEM((2, 24, LANES), jnp.float32),
            table(modes_x),
            table(modes_x),
            table(modes_y),
            table(modes_y),
            table(modes_y),
            pltpu.VMEM((GRID + LANES, slots), jnp.bfloat16),
            pltpu.VMEM((GRID + LANES, slots), jnp.bfloat16),
            pltpu.VMEM((modes_y, GRID), jnp.float32),
            pltpu.VMEM((modes_y, GRID), jnp.float32),
            pltpu.VMEM((2, modes_x, LANES), jnp.float32),
            pltpu.VMEM((modes_x * modes_y, GRID), jnp.float32),
            pltpu.VMEM((modes_x * modes_y, GRID + LANES), jnp.bfloat16),
            pltpu.VMEM((slots // LANES + 2, 8, LANES), jnp.float32),
            pltpu.SemaphoreType.DMA,
        ],
        compiler_params=pltpu.CompilerParams(vmem_limit_bytes=40 * 2**20),
    )(sites, charges, counts)


def finish_kernel(sums_ref, charge_ref, energy_ref, force_ref, landed_ref, send_sem, recv_sem):
    size_y = lax.axis_size("gy")
    me = lax.axis_index("gx") * size_y + lax.axis_index("gy")
    pl.semaphore_wait(greet_peers(), lax.axis_size("gx") * size_y - 1)
    send, land = spread_piece(lambda p: sums_ref.at[p], landed_ref, send_sem, recv_sem)
    send()
    landed_ref[me] = sums_ref[me]
    land()
    total = jnp.sum(landed_ref[...], axis=0)
    charge = charge_ref[me]
    energy_ref[0] = 0.5 * charge * total[0:1]
    for c in range(3):
        force_ref[c, 0] = -charge * total[c + 1 : c + 2]


def finish(sums, charge, collective):
    peers, rows, atoms = sums.shape
    vmem = pl.BlockSpec(memory_space=pltpu.VMEM)
    return pl.pallas_call(
        finish_kernel,
        out_shape=(
            jax.ShapeDtypeStruct((1, 1, atoms), jnp.float32),
            jax.ShapeDtypeStruct((3, 1, 1, atoms), jnp.float32),
        ),
        in_specs=[vmem, vmem],
        out_specs=(vmem, vmem),
        scratch_shapes=[
            pltpu.VMEM((peers, rows, atoms), jnp.float32),
            pltpu.SemaphoreType.DMA,
            pltpu.SemaphoreType.DMA,
        ],
        compiler_params=pltpu.CompilerParams(
            collective_id=collective, has_side_effects=True, vmem_limit_bytes=12 * 2**20
        ),
    )(sums, charge)


def local_sites(
    positions,
    neighbours,
    live_count,
    stencil_base,
    spline_weight,
    spline_slope,
    embed_scale,
    embed_bias,
    desc_gain,
    fit_in,
    fit_bias,
    fit_hidden,
    fit_bias_two,
    fit_out,
):
    sites, charges, counts = gathered_sites(
        1,
        positions,
        neighbours,
        live_count,
        stencil_base,
        spline_slope,
        embed_scale[None, :],
        embed_bias[None, :],
        desc_gain[None, :],
        fit_in.T,
        fit_bias[None, :],
        fit_hidden,
        fit_bias_two[None, :],
        fit_out[None, :],
    )
    return finish(mesh_sums(sites, charges, counts), charges, 2)


def padded_2(shard, sides, width):
    for axis, dim in sides:
        peers, length = (lax.axis_size(axis), shard.shape[dim])
        up = [(i, (i + 1) % peers) for i in range(peers)]
        down = [(j, i) for i, j in up]
        last = lax.slice_in_dim(shard, length - width, length, axis=dim)
        leading = lax.slice_in_dim(shard, 0, width, axis=dim)
        before = lax.ppermute(last, axis, up)
        after = lax.ppermute(leading, axis, down)
        shard = jnp.concatenate([before, shard, after], axis=dim)
    return shard


def shifted(block, axis, distance):
    devices = range(lax.axis_size(axis))
    route = [((i - distance) % len(devices), i) for i in devices]
    return lax.ppermute(block, axis, route)


def stencil_table(anchor, weights, length, offset, periodic):
    count = anchor.shape[0]
    cell_index = lax.broadcasted_iota(jnp.int32, (4, length, count), 1)
    tap_index = lax.broadcasted_iota(jnp.int32, (4, length, count), 0)
    target = anchor[None, None, :] + tap_index + offset
    if periodic:
        target = target % length
    chosen = jnp.where(target == cell_index, weights[:, None, :], jnp.zeros((), weights.dtype))
    return jnp.sum(chosen, axis=0)


def spread_cells(charge, anchor, weights, extent_x, extent_y, offset, length):
    table_x = stencil_table(anchor[0], weights[0] * charge[None, :], extent_x, offset, False)
    table_y = stencil_table(anchor[1], weights[1], extent_y, offset, False)
    table_z = stencil_table(anchor[2], weights[2], length, 0, True)
    planes = (table_x[:, None, :] * table_y[None, :, :]).reshape(extent_x * extent_y, -1)
    return jnp.dot(planes, table_z.T, precision=highest).reshape(extent_x, extent_y, length)


def interpolate(padded, anchor, weights, slopes):
    extent_x, extent_y, length = padded.shape
    table_x = stencil_table(anchor[0], weights[0], extent_x, 2, False)
    slope_x = stencil_table(anchor[0], slopes[0], extent_x, 2, False)
    table_y = stencil_table(anchor[1], weights[1], extent_y, 2, False)
    slope_y = stencil_table(anchor[1], slopes[1], extent_y, 2, False)
    table_z = stencil_table(anchor[2], weights[2], length, 0, True)
    slope_z = stencil_table(anchor[2], slopes[2], length, 0, True)
    flat = padded.reshape(extent_x * extent_y, length)
    along = jnp.dot(flat, table_z, precision=highest).reshape(extent_x, extent_y, -1)
    slant = jnp.dot(flat, slope_z, precision=highest).reshape(extent_x, extent_y, -1)
    over_y = jnp.sum(along * table_y[None], axis=1)
    value = jnp.sum(table_x * over_y, axis=0)
    field_x = -jnp.sum(slope_x * over_y, axis=0)
    over_x = jnp.sum(along * table_x[:, None, :], axis=0)
    field_y = -jnp.sum(slope_y * over_x, axis=0)
    slant_y = jnp.sum(slant * table_y[None], axis=1)
    field_z = -jnp.sum(table_x * slant_y, axis=0)
    return (value, jnp.stack([field_x, field_y, field_z]))


def fitted_charge(
    nearby,
    listed,
    count,
    embed_scale,
    embed_bias,
    desc_gain,
    fit_in,
    fit_bias,
    fit_hidden,
    fit_bias_two,
    fit_out,
):
    atoms = listed.shape[1]
    center = nearby[:, 4 * atoms : 5 * atoms]
    picked = jnp.take(nearby, listed.reshape(-1), axis=1).reshape(3, listed.shape[0], atoms)
    delta = picked - center[:, None, :]
    radius = jnp.sqrt(jnp.sum(delta * delta, axis=0))
    smooth = 1.0 / (1.0 + radius / radius_scale)
    factor = smooth / (radius + radius_scale)
    envelope = jnp.concatenate([smooth[None], delta * factor[None]], axis=0)
    embed = jnp.tanh(smooth[None] * embed_scale[:, None, None] + embed_bias[:, None, None])
    mixed = jnp.einsum("ekn,ckn->ecn", embed, envelope, precision=highest)
    descriptor = jnp.einsum("ecn,acn->ean", mixed, mixed[:AXIS], precision=highest).reshape(
        -1, atoms
    )
    scaling = lax.rsqrt(jnp.mean(descriptor * descriptor, axis=0) + norm_floor)
    normed = (descriptor * scaling[None, :] * desc_gain[:, None]).astype(jnp.bfloat16)
    first = jnp.tanh(
        jnp.dot(fit_in, normed, preferred_element_type=jnp.float32) + fit_bias[:, None]
    )
    second = (
        jnp.tanh(
            jnp.dot(fit_hidden, first.astype(jnp.bfloat16), preferred_element_type=jnp.float32)
            + fit_bias_two[:, None]
        )
        + first
    )
    charge = jnp.sum(fit_out[:, None] * second, axis=0)
    slot_index = lax.broadcasted_iota(jnp.int32, (atoms,), 0)
    return jnp.where(slot_index < count, charge, jnp.zeros((), charge.dtype))


def wave_number(index, length):
    signed = jnp.where(index > length // 2, index - length, index)
    return signed.astype(jnp.float32) * (full_turn / length)


def green_values(index_x, index_y, index_z, length):
    wave_x = wave_number(index_x, length)
    wave_y = wave_number(index_y, length)
    wave_z = wave_number(index_z, length)
    square = wave_x * wave_x + wave_y * wave_y + wave_z * wave_z
    safe = jnp.where(square > 0, square, 1.0)
    value = 2.0 * full_turn * jnp.exp(-0.5 * screen_width * screen_width * square) / safe
    keep = (square > 0) & (index_z != length // 2)
    return jnp.where(keep, value, 0.0)


def wave_tables(length, count):
    rows = lax.broadcasted_iota(jnp.int32, (length, count), 0)
    cols = lax.broadcasted_iota(jnp.int32, (length, count), 1)
    angle = (rows * cols % length).astype(jnp.float32) * (full_turn / length)
    return (jnp.cos(angle), jnp.sin(angle))


def along_axis(real_part, imag_part, cosine, sine, sign, form):
    real_cos = jnp.einsum(form, real_part, cosine, precision=highest)
    real_sin = jnp.einsum(form, real_part, sine, precision=highest)
    imag_cos = jnp.einsum(form, imag_part, cosine, precision=highest)
    imag_sin = jnp.einsum(form, imag_part, sine, precision=highest)
    return (real_cos + sign * imag_sin, imag_cos - sign * real_sin)


def local_mesh(
    positions,
    neighbours,
    live_count,
    stencil_base,
    spline_weight,
    spline_slope,
    embed_scale,
    embed_bias,
    desc_gain,
    fit_in,
    fit_bias,
    fit_hidden,
    fit_bias_two,
    fit_out,
):
    columns_y = lax.axis_size("gy")
    width_x = GRID // lax.axis_size("gx")
    width_y = GRID // columns_y
    atoms = positions.shape[3]
    beside_all = padded_2(positions, (("gx", 1), ("gy", 2)), 1)
    block_x = lax.broadcasted_iota(jnp.int32, (3, 3, atoms), 0) - 1
    block_y = lax.broadcasted_iota(jnp.int32, (3, 3, atoms), 1) - 1
    offsets = jnp.stack([block_x * width_x, block_y * width_y, jnp.zeros_like(block_x)]).astype(
        jnp.float32
    )
    nearby = (beside_all + offsets).reshape(3, 9 * atoms)
    charge = fitted_charge(
        nearby,
        neighbours[:, 0, 0, :],
        live_count[0, 0],
        embed_scale,
        embed_bias,
        desc_gain,
        fit_in,
        fit_bias,
        fit_hidden,
        fit_bias_two,
        fit_out,
    )
    anchor = stencil_base[:, 0, 0, :]
    weights = spline_weight[:, :, 0, 0, :]
    slopes = spline_slope[:, :, 0, 0, :]
    spread = spread_cells(charge, anchor, weights, width_x + 4, width_y + 4, 2, GRID)
    inner = spread[2 : width_x + 2]
    for stride in (1, -1):
        piece = spread[width_x + 2 :] if stride == 1 else spread[:2]
        moved = shifted(piece, "gx", stride)
        if stride == 1:
            inner = inner.at[:2].add(moved)
        else:
            inner = inner.at[width_x - 2 :].add(moved)
    density = inner[:, 2 : width_y + 2]
    for stride in (1, -1):
        piece = inner[:, width_y + 2 :] if stride == 1 else inner[:, :2]
        moved = shifted(piece, "gy", stride)
        if stride == 1:
            density = density.at[:, :2].add(moved)
        else:
            density = density.at[:, width_y - 2 :].add(moved)
    freqs = GRID // 2
    fold_weight = jnp.where(jnp.arange(freqs) == 0, 1.0, 2.0).astype(jnp.float32) / GRID
    cosine_z, sine_z = wave_tables(GRID, freqs)
    flat = density.reshape(width_x * width_y, GRID)
    real_part = jnp.dot(flat, cosine_z, precision=highest).reshape(width_x, width_y, freqs)
    imag_part = -jnp.dot(flat, sine_z, precision=highest).reshape(width_x, width_y, freqs)
    real_part, imag_part = (
        lax.all_to_all(real_part, "gy", split_axis=2, concat_axis=1, tiled=True),
        lax.all_to_all(imag_part, "gy", split_axis=2, concat_axis=1, tiled=True),
    )
    cosine, sine = wave_tables(GRID, GRID)
    real_part, imag_part = along_axis(real_part, imag_part, cosine, sine, 1.0, "xym,yk->xkm")
    real_part, imag_part = (
        lax.all_to_all(real_part, "gx", split_axis=1, concat_axis=0, tiled=True),
        lax.all_to_all(imag_part, "gx", split_axis=1, concat_axis=0, tiled=True),
    )
    real_part, imag_part = along_axis(real_part, imag_part, cosine, sine, 1.0, "xym,xk->kym")
    span_y = real_part.shape[1]
    span_z = real_part.shape[2]
    index_x = lax.broadcasted_iota(jnp.int32, (GRID, span_y, span_z), 0)
    index_y = lax.axis_index("gx") * span_y + lax.broadcasted_iota(
        jnp.int32, (GRID, span_y, span_z), 1
    )
    index_z = lax.axis_index("gy") * span_z + lax.broadcasted_iota(
        jnp.int32, (GRID, span_y, span_z), 2
    )
    green = green_values(index_x, index_y, index_z, GRID)
    real_part = real_part * green
    imag_part = imag_part * green
    back_cos = cosine / GRID
    back_sin = sine / GRID
    real_part, imag_part = along_axis(real_part, imag_part, back_cos, back_sin, -1.0, "xym,xk->kym")
    real_part, imag_part = (
        lax.all_to_all(real_part, "gx", split_axis=0, concat_axis=1, tiled=True),
        lax.all_to_all(imag_part, "gx", split_axis=0, concat_axis=1, tiled=True),
    )
    real_part, imag_part = along_axis(real_part, imag_part, back_cos, back_sin, -1.0, "xym,yk->xkm")
    real_part, imag_part = (
        lax.all_to_all(real_part, "gy", split_axis=1, concat_axis=2, tiled=True),
        lax.all_to_all(imag_part, "gy", split_axis=1, concat_axis=2, tiled=True),
    )
    rows_y = real_part.shape[1]
    flat_real = real_part.reshape(width_x * rows_y, freqs)
    flat_imag = imag_part.reshape(width_x * rows_y, freqs)
    summed_cos = (cosine_z * fold_weight[None, :]).T
    summed_sin = (sine_z * fold_weight[None, :]).T
    potential = jnp.dot(flat_real, summed_cos, precision=highest) - jnp.dot(
        flat_imag, summed_sin, precision=highest
    )
    potential = potential.reshape(width_x, rows_y, GRID)
    padded = padded_2(potential, (("gx", 0), ("gy", 1)), 2)
    value, field = interpolate(padded, anchor, weights, slopes)
    energy = (0.5 * charge * value).reshape(1, 1, atoms)
    force = (charge[None, :] * field).reshape(3, 1, 1, atoms)
    return (energy, force)


def solution(mesh):
    def local(positions, *rest):
        columns_x, columns_y = (lax.axis_size("gx"), lax.axis_size("gy"))
        sites = columns_x * columns_y * positions.shape[3]
        whole = GRID % (16 * columns_x) == 0 and GRID % (16 * columns_y) == 0
        few = whole and sites <= 8 * GRID * 2
        return (local_sites if few and positions.shape[3] == LANES else local_mesh)(positions, *rest)

    placed = (
        P(None, "gx", "gy", None),
        P(None, "gx", "gy", None),
        P("gx", "gy"),
        P(None, "gx", "gy", None),
        P(None, None, "gx", "gy", None),
        P(None, None, "gx", "gy", None),
        P(),
        P(),
        P(),
        P(),
        P(),
        P(),
        P(),
        P(),
    )
    return jax.shard_map(
        local,
        mesh=mesh,
        in_specs=placed,
        out_specs=(P("gx", "gy", None), P(None, "gx", "gy", None)),
        check_vma=False,
    )
```

```python
import math

import jax
import jax.numpy as jnp
from jax import lax
from jax.experimental import pallas as pl
from jax.experimental.pallas import tpu as pltpu
from jax.sharding import PartitionSpec as P

GRID = 384
AXIS = 16
LANES = 128
CHUNK = 256
TILE = 256
FINE = (5, 13)

highest = lax.Precision.HIGHEST
radius_scale = 4.0
screen_width = 0.25
norm_floor = 1e-06
full_turn = 2.0 * math.pi


def each_peer(visit):
    size_x = lax.axis_size("gx")
    size_y = lax.axis_size("gy")
    place_x = lax.axis_index("gx")
    place_y = lax.axis_index("gy")
    across = [(place_y + b) % size_y for b in range(size_y)]
    for b in range(1, size_y):
        visit(b, place_x, across[b])

    def row(a, carry):
        x = (place_x + a) % size_x
        for b in range(size_y):
            visit(a * size_y + b, x, across[b])
        return carry

    lax.fori_loop(1, size_x, row, 0)


def greet_peers():
    barrier = pltpu.get_barrier_semaphore()

    def greet(k, x, y):
        pl.semaphore_signal(
            barrier, inc=1, device_id=(x, y), device_id_type=pl.DeviceIdType.MESH
        )

    each_peer(greet)
    return barrier


def spread_piece(piece, whole_ref, send_sem, recv_sem):
    size_y = lax.axis_size("gy")
    peers = lax.axis_size("gx") * size_y
    me = lax.axis_index("gx") * size_y + lax.axis_index("gy")

    def send(k, x, y):
        pltpu.make_async_remote_copy(
            src_ref=piece(x * size_y + y),
            dst_ref=whole_ref.at[me],
            send_sem=send_sem,
            recv_sem=recv_sem,
            device_id=(x, y),
            device_id_type=pl.DeviceIdType.MESH,
        ).start()

    def land():
        others = whole_ref.at[pl.ds(0, peers - 1)]
        pltpu.make_async_copy(others, others, send_sem).wait()
        pltpu.make_async_copy(others, others, recv_sem).wait()

    return (lambda: each_peer(send)), land


def column(table, index, length):
    return jnp.broadcast_to(table[:length, index : index + 1], (length, LANES))


def site_kernel(
    position_ref,
    neighbour_ref,
    count_ref,
    base_ref,
    slope_ref,
    scale_ref,
    bias_ref,
    gain_ref,
    fit_in_hbm,
    fit_bias_ref,
    fit_hidden_hbm,
    fit_bias_two_ref,
    fit_out_ref,
    sites_ref,
    charges_ref,
    counts_ref,
    place_ref,
    parcel_ref,
    own_ref,
    near_ref,
    listed_ref,
    rows_ref,
    columns_ref,
    gains_ref,
    env_ref,
    mixed_ref,
    descriptor_ref,
    normed_ref,
    fit_in_ref,
    fit_hidden_ref,
    load_sem,
    near_send,
    near_recv,
    site_send,
    site_recv,
    charge_send,
    charge_recv,
):
    size_x = lax.axis_size("gx")
    size_y = lax.axis_size("gy")
    peers = size_x * size_y
    place_x = lax.axis_index("gx")
    place_y = lax.axis_index("gy")
    me = place_x * size_y + place_y
    width_x = GRID // size_x
    width_y = GRID // size_y
    neigh = neighbour_ref.shape[0]
    atoms = neighbour_ref.shape[3]
    width = scale_ref.shape[1]
    features = gain_ref.shape[1]
    loads = [
        pltpu.make_async_copy(fit_in_hbm, fit_in_ref, load_sem.at[0]),
        pltpu.make_async_copy(fit_hidden_hbm, fit_hidden_ref, load_sem.at[1]),
    ]
    for load in loads:
        load.start()
    barrier = greet_peers()

    count = count_ref[0, 0]
    origin = (place_x * width_x + 1, place_y * width_y + 1, 1)
    place_ref[...] = jnp.zeros_like(place_ref)
    for c in range(3):
        place_ref[c : c + 1, :] = position_ref[c, 0]
        part = slope_ref[c, 0, 0] + slope_ref[c, 3, 0] + 0.5
        parcel_ref[c : c + 1, :] = (base_ref[c, 0] + origin[c]).astype(jnp.float32) + part
    parcel_ref[3:4, :] = jnp.full((1, atoms), count, jnp.int32).astype(jnp.float32)
    for k in range(neigh):
        listed_ref[k : k + 1, :] = neighbour_ref[k, 0]

    pl.semaphore_wait(barrier, peers - 1)

    def near_copy(slot, target):
        return pltpu.make_async_remote_copy(
            src_ref=place_ref,
            dst_ref=near_ref.at[slot],
            send_sem=near_send,
            recv_sem=near_recv,
            device_id=target,
            device_id_type=pl.DeviceIdType.MESH,
        )

    around = [(a, b) for a in (-1, 0, 1) for b in (-1, 0, 1)]
    targets = [((place_x - a) % size_x, (place_y - b) % size_y) for a, b in around]
    for slot in range(9):
        if slot != 4:
            near_copy(slot, targets[slot]).start()

    send_sites, land_sites = spread_piece(lambda p: parcel_ref, sites_ref, site_send, site_recv)
    send_sites()
    near_ref[4] = place_ref[...]
    sites_ref[me] = parcel_ref[...]

    rows_ref[...] = jnp.zeros_like(rows_ref)
    for index, ref in enumerate((scale_ref, bias_ref)):
        rows_ref[index : index + 1, :width] = ref[...]
    for index, ref in enumerate((fit_bias_ref, fit_bias_two_ref, fit_out_ref)):
        rows_ref[index + 2 : index + 3, :] = ref[...]
    parts = -(-features // LANES)
    for part in range(parts):
        size = min(LANES, features - part * LANES)
        rows_ref[part + 5 : part + 6, :size] = gain_ref[:, part * LANES : part * LANES + size]
    columns_ref[...] = rows_ref[...].T
    for part in range(parts):
        size = min(LANES, features - part * LANES)
        gains_ref[part * LANES : part * LANES + size, :] = column(columns_ref, part + 5, size)

    others = near_ref.at[pl.ds(0, 8)]
    pltpu.make_async_copy(others, others, near_send).wait()
    pltpu.make_async_copy(others, others, near_recv).wait()

    listed = listed_ref[...]
    slots = listed % atoms
    blocks = listed // atoms
    square = jnp.zeros((neigh, atoms), jnp.float32)
    deltas = []
    for c in range(3):
        center = near_ref[4, c : c + 1, :]
        picked = jnp.zeros((neigh, atoms), jnp.float32)
        for slot, (a, b) in enumerate(around):
            offset = (a * width_x, b * width_y, 0)[c]
            row = jnp.broadcast_to(near_ref[slot, c : c + 1, :] + float(offset), (neigh, atoms))
            got = jnp.take_along_axis(row, slots, axis=1, mode="promise_in_bounds")
            picked = jnp.where(blocks == slot, got, picked)
        delta = picked - center
        deltas.append(delta)
        square = square + delta * delta
    radius = jnp.sqrt(square)
    smooth = 1.0 / (1.0 + radius / radius_scale)
    factor = smooth / (radius + radius_scale)
    env_ref[0] = smooth
    for c in range(3):
        env_ref[c + 1] = deltas[c] * factor

    padded = mixed_ref.shape[1]
    bounds = [(0, padded // 16 * 8), (padded // 16 * 8, padded)]
    for first, last in bounds:
        span = last - first
        scale = jnp.broadcast_to(columns_ref[first:last, 0:1], (span, atoms))
        shift = jnp.broadcast_to(columns_ref[first:last, 1:2], (span, atoms))

        def step(k, sums):
            rows = [env_ref[c, pl.ds(k, 1), :] for c in range(4)]
            embed = jnp.tanh(rows[0] * scale + shift)
            return tuple(total + embed * row for total, row in zip(sums, rows))

        zero = jnp.zeros((span, atoms), jnp.float32)
        sums = lax.fori_loop(0, neigh, step, (zero, zero, zero, zero), unroll=2)
        for c in range(4):
            mixed_ref[c, first:last, :] = sums[c]

    def describe(e, total):
        value = jnp.zeros((AXIS, atoms), jnp.float32)
        for c in range(4):
            value = value + mixed_ref[c, pl.ds(e, 1), :] * mixed_ref[c, :AXIS, :]
        descriptor_ref[pl.ds(pl.multiple_of(e * AXIS, AXIS), AXIS), :] = value
        return total + value * value

    total = lax.fori_loop(0, width, describe, jnp.zeros((AXIS, atoms), jnp.float32), unroll=10)
    mean = jnp.sum(total, axis=0, keepdims=True) / features
    scaling = lax.rsqrt(mean + norm_floor)
    normed_ref[...] = (descriptor_ref[...] * scaling * gains_ref[...]).astype(jnp.bfloat16)
    for load in loads:
        load.wait()
    first = lax.dot_general(
        fit_in_ref[...],
        normed_ref[...],
        (((0,), (0,)), ((), ())),
        preferred_element_type=jnp.float32,
    )
    first = jnp.tanh(first + column(columns_ref, 2, LANES))
    second = jnp.dot(
        fit_hidden_ref[...], first.astype(jnp.bfloat16), preferred_element_type=jnp.float32
    )
    second = jnp.tanh(second + column(columns_ref, 3, LANES)) + first
    charge = jnp.sum(column(columns_ref, 4, LANES) * second, axis=0, keepdims=True)
    lane = lax.broadcasted_iota(jnp.int32, (1, atoms), 1)
    own_ref[...] = jnp.where(lane < count, charge, 0.0)

    send_charges, land_charges = spread_piece(
        lambda p: own_ref, charges_ref, charge_send, charge_recv
    )
    send_charges()
    charges_ref[me] = own_ref[...]
    land_sites()
    for p in range(peers):
        counts_ref[p : p + 1, :] = sites_ref[p, 3:4, :].astype(jnp.int32)
    land_charges()


def gathered_sites(collective, *args):
    peers = lax.axis_size("gx") * lax.axis_size("gy")
    neigh = args[1].shape[0]
    atoms = args[1].shape[3]
    width = args[5].shape[1]
    features = args[7].shape[1]
    padded = -(-width // 8) * 8
    vmem = pl.BlockSpec(memory_space=pltpu.VMEM)
    smem = pl.BlockSpec(memory_space=pltpu.SMEM)
    hbm = pl.BlockSpec(memory_space=pltpu.HBM)
    dma = pltpu.SemaphoreType.DMA
    return pl.pallas_call(
        site_kernel,
        in_specs=[vmem, vmem, smem] + [vmem] * 5 + [hbm, vmem, hbm, vmem, vmem],
        out_specs=(vmem, vmem, vmem),
        out_shape=(
            jax.ShapeDtypeStruct((peers, 4, atoms), jnp.float32),
            jax.ShapeDtypeStruct((peers, 1, atoms), jnp.float32),
            jax.ShapeDtypeStruct((peers, atoms), jnp.int32),
        ),
        scratch_shapes=[
            pltpu.VMEM((4, atoms), jnp.float32),
            pltpu.VMEM((4, atoms), jnp.float32),
            pltpu.VMEM((1, atoms), jnp.float32),
            pltpu.VMEM((9, 4, atoms), jnp.float32),
            pltpu.VMEM((neigh, atoms), jnp.int32),
            pltpu.VMEM((LANES, LANES), jnp.float32),
            pltpu.VMEM((LANES, LANES), jnp.float32),
            pltpu.VMEM((features, atoms), jnp.float32),
            pltpu.VMEM((4, neigh, atoms), jnp.float32),
            pltpu.VMEM((4, padded, atoms), jnp.float32),
            pltpu.VMEM((features, atoms), jnp.float32),
            pltpu.VMEM((features, atoms), jnp.bfloat16),
            pltpu.VMEM(args[8].shape, args[8].dtype),
            pltpu.VMEM(args[10].shape, args[10].dtype),
            dma((2,)),
            dma,
            dma,
            dma,
            dma,
            dma,
            dma,
        ],
        compiler_params=pltpu.CompilerParams(
            collective_id=collective, has_side_effects=True, vmem_limit_bytes=12 * 2**20
        ),
    )(*args)


def sine(index):
    angle = index * (full_turn / GRID)
    square = angle * angle
    total = jnp.full_like(square, -1.0 / 39916800.0)
    for term in (1.0 / 362880.0, -1.0 / 5040.0, 1.0 / 120.0, -1.0 / 6.0, 1.0):
        total = total * square + term
    return total * angle


def turned(index):
    index = index - GRID * jnp.floor(index * (1.0 / GRID))
    signed = index - GRID // 2
    size = jnp.abs(signed)
    near = jnp.minimum(size, GRID // 2 - size)
    return sine(size - GRID // 4), sine(jnp.where(signed < 0, near, -near))


def spline_taps(part):
    rest = 1.0 - part
    square = part * part
    cube = square * part
    weights = (
        rest * rest * rest * (1.0 / 6.0),
        (3.0 * cube - 6.0 * square + 4.0) * (1.0 / 6.0),
        (-3.0 * cube + 3.0 * square + 3.0 * part + 1.0) * (1.0 / 6.0),
        cube * (1.0 / 6.0),
    )
    slopes = (
        -0.5 * rest * rest,
        (3.0 * square - 4.0 * part) * 0.5,
        (-3.0 * square + 2.0 * part + 1.0) * 0.5,
        0.5 * square,
    )
    return weights, slopes


def mode_pairs(taps, wave):
    (cos_one, sin_one, cos_two, sin_two), (cosine, sine_part) = wave
    real = taps[1] + (taps[0] + taps[2]) * cos_one + taps[3] * cos_two
    imag = (taps[2] - taps[0]) * sin_one + taps[3] * sin_two
    return cosine * real - sine_part * imag, sine_part * real + cosine * imag


def field_kernel(
    sites_ref,
    charges_ref,
    listed_ref,
    out_ref,
    count_ref,
    packed_ref,
    wave_ref,
    high_ref,
    x_ref,
    slope_x_ref,
    y_ref,
    slope_y_ref,
    lit_ref,
    z_ref,
    slope_z_ref,
    plane_ref,
    weight_ref,
    row_ref,
    spectrum_ref,
    scaled_ref,
    found_ref,
    sem,
):
    size_x = lax.axis_size("gx")
    size_y = lax.axis_size("gy")
    columns = size_x * size_y
    modes_x = x_ref.shape[0]
    modes_y = y_ref.shape[0]
    modes_z = spectrum_ref.shape[1]
    half_x = modes_x // 2
    half_y = modes_y // 2
    half_z = modes_z // 2
    start_x = lax.axis_index("gx") * half_x
    start_y = lax.axis_index("gy") * half_y
    group = modes_x
    shape = (8, LANES)
    copy = pltpu.make_async_copy(listed_ref, count_ref, sem)
    copy.start()

    spectrum_ref[...] = jnp.zeros_like(spectrum_ref)
    found_ref[...] = jnp.zeros_like(found_ref)
    packed_ref[...] = jnp.zeros_like(packed_ref)
    sub = lax.broadcasted_iota(jnp.int32, shape, 0).astype(jnp.float32)
    lane = lax.broadcasted_iota(jnp.int32, shape, 1)
    starts = [start_x.astype(jnp.float32), start_y.astype(jnp.float32), 0.0]
    groups = [half_x // 8, half_y // 8, half_z // 8]
    firsts = [0, groups[0], groups[0] + groups[1]]
    for d in range(3):
        rows = groups[d] * 8
        mode = lax.broadcasted_iota(jnp.int32, (rows, LANES), 0).astype(jnp.float32) + starts[d]
        cosine, sine_part = turned(mode)
        double = (1.0 - 2.0 * sine_part * sine_part, 2.0 * sine_part * cosine)
        for index, value in enumerate((cosine, sine_part) + double):
            wave_ref[firsts[d] : firsts[d] + groups[d], index] = value.reshape(groups[d], 8, LANES)

    fine = LANES // 2
    spot = lax.broadcasted_iota(jnp.int32, (modes_y, modes_z), 1)
    rest = jnp.where(spot < LANES, spot, (spot - LANES) % (half_z - fine))
    mode = jnp.where(
        spot < LANES, FINE[0] * 8 + spot % fine, jnp.where(rest < FINE[0] * 8, rest, rest + fine)
    ).astype(jnp.float32)
    factor = jnp.where(mode == 0, 1.0, 2.0) * (1.0 / GRID)
    wave = mode * (full_turn / GRID)
    square = wave * wave
    spot = lax.broadcasted_iota(jnp.int32, (modes_y, modes_z), 0)
    mode = start_y + jnp.where(spot < half_y, spot, spot - half_y)
    mode = jnp.where((mode == 0) & (spot >= half_y), GRID // 2, mode)
    ends = (mode == 0) | (mode == GRID // 2)
    factor = factor * jnp.where(ends, 1.0, 2.0) * (1.0 / GRID)
    wave = mode.astype(jnp.float32) * (full_turn / GRID)
    square = square + wave * wave
    decay = -0.5 * screen_width * screen_width
    plane_ref[...] = square
    weight_ref[...] = jnp.exp(square * decay) * factor * (2.0 * full_turn)
    spot = lax.broadcasted_iota(jnp.int32, (modes_x, LANES), 0)
    mode = start_x + jnp.where(spot < half_x, spot, spot - half_x)
    mode = jnp.where((mode == 0) & (spot >= half_x), GRID // 2, mode)
    ends = (mode == 0) | (mode == GRID // 2)
    wave = mode.astype(jnp.float32) * (full_turn / GRID)
    square = wave * wave
    row_ref[0] = square
    row_ref[1] = jnp.exp(square * decay) * jnp.where(ends, 1.0, 2.0) * (1.0 / GRID)

    copy.wait()

    def pack(j, start):
        count = count_ref[j, 0]
        tile = start // LANES
        shift = start % LANES
        site = jnp.concatenate([sites_ref[j], jnp.broadcast_to(charges_ref[j], (4, LANES))], axis=0)
        turn = pltpu.roll(jnp.where(lane < count, site, 0.0), shift, 1)
        packed_ref[tile] = packed_ref[tile] + jnp.where(lane >= shift, turn, 0.0)
        packed_ref[tile + 1] = jnp.where(lane < shift, turn, 0.0)
        return start + count

    total = lax.fori_loop(0, columns, pack, 0, unroll=4)
    chunks = (total + CHUNK - 1) // CHUNK
    order = list(range(*FINE)) + list(range(FINE[0])) + list(range(FINE[1], groups[2]))

    def tables(tile, carry):
        lanes = pl.ds(pl.multiple_of(tile * LANES, LANES), LANES)
        charge = jnp.broadcast_to(packed_ref[tile, 7:8, :], shape)
        for d in range(3):
            spot = jnp.broadcast_to(packed_ref[tile, d : d + 1, :], shape)
            cell = jnp.floor(spot)
            part = spot - cell
            weights, slopes = spline_taps(part)
            low_cos, low_sin = turned(sub * cell)
            for h in range(-(-groups[d] // 8)):
                high_cos, high_sin = turned((starts[d] + 8.0 * (sub + 8.0 * h)) * cell)
                high_ref[0, 8 * h : 8 * h + 8] = high_cos
                high_ref[1, 8 * h : 8 * h + 8] = high_sin

            def pairs(g):
                high_cos = high_ref[0, g : g + 1]
                high_sin = high_ref[1, g : g + 1]
                constants = tuple(wave_ref[firsts[d] + g, index] for index in range(4))
                wave = (
                    constants,
                    (
                        high_cos * low_cos - high_sin * low_sin,
                        high_sin * low_cos + high_cos * low_sin,
                    ),
                )
                return mode_pairs(weights, wave) + mode_pairs(slopes, wave)

            if d < 2:
                half = groups[d] * 8
                for g in range(groups[d]):
                    even, odd, slope_even, slope_odd = pairs(g)
                    if g == 0:
                        parity = cell - 2.0 * jnp.floor(cell * 0.5)
                        parity = 1.0 - 2.0 * parity
                        first = (sub + starts[d]) == 0
                        last = parity * (weights[1] + weights[3] - weights[0] - weights[2])
                        odd = jnp.where(first, last, odd)
                        last = parity * (slopes[1] + slopes[3] - slopes[0] - slopes[2])
                        slope_odd = jnp.where(first, last, slope_odd)
                    table = (x_ref, y_ref)[d]
                    slope = (slope_x_ref, slope_y_ref)[d]
                    table[8 * g : 8 * g + 8, lanes] = even
                    table[half + 8 * g : half + 8 * g + 8, lanes] = odd
                    slope[8 * g : 8 * g + 8, lanes] = slope_even
                    slope[half + 8 * g : half + 8 * g + 8, lanes] = slope_odd
                    if d == 1:
                        lit_ref[8 * g : 8 * g + 8, lanes] = even * charge
                        lit_ref[half + 8 * g : half + 8 * g + 8, lanes] = odd * charge
                continue
            for index in range(0, len(order), 2):
                both = [pairs(order[index]), pairs(order[index + 1])]
                fine_part = index < FINE[1] - FINE[0]
                if fine_part:
                    spots = (8 * index, fine + 8 * index)
                else:
                    spots = (LANES + 8 * index - fine, half_z + 8 * index)
                for which in range(4):
                    table = z_ref if which < 2 else slope_z_ref
                    value = jnp.concatenate([both[0][which], both[1][which]], axis=0)
                    high = value.astype(jnp.bfloat16)
                    row = spots[which % 2]
                    table[row : row + 16, lanes] = high
                    if fine_part:
                        low = value - high.astype(jnp.float32)
                        row = row + modes_z
                        table[row : row + 16, lanes] = low.astype(jnp.bfloat16)
        return carry

    lax.fori_loop(0, chunks * (CHUNK // LANES), tables, 0)

    def gather_chunk(chunk, carry):
        lanes = pl.ds(pl.multiple_of(chunk * CHUNK, CHUNK), CHUNK)
        y = lit_ref[:, lanes]
        z = z_ref[:, lanes]

        def rows(g, inner):
            x = x_ref[pl.ds(pl.multiple_of(g * group, group), group), lanes]
            left = jnp.concatenate(
                [(x[a : a + 1] * y).astype(jnp.bfloat16) for a in range(group)], axis=0
            )
            where = pl.ds(pl.multiple_of(g * group * modes_y, group * modes_y), group * modes_y)
            form = (((1,), (1,)), ((), ()))
            both = lax.dot_general(left, z, form, preferred_element_type=jnp.float32)
            spectrum_ref[where, :LANES] += both[:, :LANES] + both[:, modes_z:]
            spectrum_ref[where, LANES:] += both[:, LANES:modes_z]
            return inner

        return lax.fori_loop(0, modes_x // group, rows, carry)

    lax.fori_loop(0, chunks, gather_chunk, 0)

    def spread(row):
        return jnp.concatenate([row] * (modes_z // LANES), axis=1)

    def apply(a, square, weight):
        green = weight / square * spread(row_ref[1, pl.ds(a, 1), :])
        where = pl.ds(pl.multiple_of(a * modes_y, modes_y), modes_y)
        value = (spectrum_ref[where, :] * green).astype(jnp.bfloat16)
        scaled_ref[where, :modes_z] = value
        scaled_ref[where, modes_z:] = value[:, :LANES]

    square = plane_ref[...] + spread(row_ref[0, 0:1, :])
    above = square > 0
    apply(0, jnp.where(above, square, 1.0), jnp.where(above, weight_ref[...], 0.0))

    def scale(a, carry):
        apply(a, plane_ref[...] + spread(row_ref[0, pl.ds(a, 1), :]), weight_ref[...])
        return carry

    lax.fori_loop(1, modes_x, scale, 0, unroll=2)

    def site_sums(block, width):
        lanes = pl.ds(pl.multiple_of(block * LANES, width), width)
        y = y_ref[:, lanes]
        slope_y = slope_y_ref[:, lanes]
        x = x_ref[:, lanes]
        slope_x = slope_x_ref[:, lanes]
        paired = jnp.concatenate([z_ref[:, lanes], slope_z_ref[:, lanes]], axis=1)
        both = jnp.dot(scaled_ref[...], paired, preferred_element_type=jnp.float32)
        value = field_x = field_y = field_z = jnp.zeros((8, width), jnp.float32)
        for a in range(modes_x):
            part = both[a * modes_y : (a + 1) * modes_y, :width]
            skew = both[a * modes_y : (a + 1) * modes_y, width:]
            over = jnp.sum((part * y).reshape(modes_y // 8, 8, width), axis=0)
            tilt = jnp.sum((part * slope_y).reshape(modes_y // 8, 8, width), axis=0)
            deep = jnp.sum((skew * y).reshape(modes_y // 8, 8, width), axis=0)
            row = x[a : a + 1]
            value = value + over * row
            field_x = field_x + over * slope_x[a : a + 1]
            field_y = field_y + tilt * row
            field_z = field_z + deep * row
        for part in range(width // LANES):
            for c, found in enumerate((value, field_x, field_y, field_z)):
                found_ref[block + part, c : c + 1, :] = jnp.sum(
                    found[:, part * LANES : (part + 1) * LANES], axis=0, keepdims=True
                )

    def tile_step(tile, carry):
        site_sums(tile * (TILE // LANES), TILE)
        return carry

    blocks = (total + LANES - 1) // LANES
    pairs_of = blocks // (TILE // LANES)
    lax.fori_loop(0, pairs_of, tile_step, 0)

    @pl.when(blocks % (TILE // LANES) > 0)
    def _():
        site_sums(pairs_of * (TILE // LANES), LANES)

    def place(j, start):
        tile = start // LANES
        shift = start % LANES
        back = (LANES - shift) % LANES
        first = pltpu.roll(found_ref[tile], back, 1)
        second = pltpu.roll(found_ref[tile + 1], back, 1)
        out_ref[j] = jnp.where(lane < LANES - shift, first, second)[:4]
        return start + count_ref[j, 0]

    lax.fori_loop(0, columns, place, 0, unroll=4)


def mesh_sums(sites, charges, counts):
    size_x = lax.axis_size("gx")
    size_y = lax.axis_size("gy")
    columns, _, atoms = sites.shape
    slots = -(-(columns * atoms) // CHUNK) * CHUNK
    modes_x = GRID // size_x
    modes_y = GRID // size_y
    groups = (modes_x + modes_y + GRID) // 16
    vmem = pl.BlockSpec(memory_space=pltpu.VMEM)
    table = lambda rows: pltpu.VMEM((rows, slots), jnp.float32)
    return pl.pallas_call(
        field_kernel,
        in_specs=[vmem, vmem, vmem],
        out_specs=vmem,
        out_shape=jax.ShapeDtypeStruct((columns, 4, atoms), jnp.float32),
        scratch_shapes=[
            pltpu.SMEM(counts.shape, jnp.int32),
            pltpu.VMEM((slots // LANES + 2, 8, LANES), jnp.float32),
            pltpu.VMEM((groups, 4, 8, LANES), jnp.float32),
            pltpu.VMEM((2, 24, LANES), jnp.float32),
            table(modes_x),
            table(modes_x),
            table(modes_y),
            table(modes_y),
            table(modes_y),
            pltpu.VMEM((GRID + LANES, slots), jnp.bfloat16),
            pltpu.VMEM((GRID + LANES, slots), jnp.bfloat16),
            pltpu.VMEM((modes_y, GRID), jnp.float32),
            pltpu.VMEM((modes_y, GRID), jnp.float32),
            pltpu.VMEM((2, modes_x, LANES), jnp.float32),
            pltpu.VMEM((modes_x * modes_y, GRID), jnp.float32),
            pltpu.VMEM((modes_x * modes_y, GRID + LANES), jnp.bfloat16),
            pltpu.VMEM((slots // LANES + 2, 8, LANES), jnp.float32),
            pltpu.SemaphoreType.DMA,
        ],
        compiler_params=pltpu.CompilerParams(vmem_limit_bytes=40 * 2**20),
    )(sites, charges, counts)


def finish_kernel(sums_ref, charge_ref, energy_ref, force_ref, landed_ref, send_sem, recv_sem):
    size_y = lax.axis_size("gy")
    me = lax.axis_index("gx") * size_y + lax.axis_index("gy")
    pl.semaphore_wait(greet_peers(), lax.axis_size("gx") * size_y - 1)
    send, land = spread_piece(lambda p: sums_ref.at[p], landed_ref, send_sem, recv_sem)
    send()
    landed_ref[me] = sums_ref[me]
    land()
    total = jnp.sum(landed_ref[...], axis=0)
    charge = charge_ref[me]
    energy_ref[0] = 0.5 * charge * total[0:1]
    for c in range(3):
        force_ref[c, 0] = -charge * total[c + 1 : c + 2]


def finish(sums, charge, collective):
    peers, rows, atoms = sums.shape
    vmem = pl.BlockSpec(memory_space=pltpu.VMEM)
    return pl.pallas_call(
        finish_kernel,
        out_shape=(
            jax.ShapeDtypeStruct((1, 1, atoms), jnp.float32),
            jax.ShapeDtypeStruct((3, 1, 1, atoms), jnp.float32),
        ),
        in_specs=[vmem, vmem],
        out_specs=(vmem, vmem),
        scratch_shapes=[
            pltpu.VMEM((peers, rows, atoms), jnp.float32),
            pltpu.SemaphoreType.DMA,
            pltpu.SemaphoreType.DMA,
        ],
        compiler_params=pltpu.CompilerParams(
            collective_id=collective, has_side_effects=True, vmem_limit_bytes=12 * 2**20
        ),
    )(sums, charge)


def local_sites(
    positions,
    neighbours,
    live_count,
    stencil_base,
    spline_weight,
    spline_slope,
    embed_scale,
    embed_bias,
    desc_gain,
    fit_in,
    fit_bias,
    fit_hidden,
    fit_bias_two,
    fit_out,
):
    sites, charges, counts = gathered_sites(
        1,
        positions,
        neighbours,
        live_count,
        stencil_base,
        spline_slope,
        embed_scale[None, :],
        embed_bias[None, :],
        desc_gain[None, :],
        fit_in.T,
        fit_bias[None, :],
        fit_hidden,
        fit_bias_two[None, :],
        fit_out[None, :],
    )
    return finish(mesh_sums(sites, charges, counts), charges, 2)


def padded_2(shard, sides, width):
    for axis, dim in sides:
        peers, length = (lax.axis_size(axis), shard.shape[dim])
        up = [(i, (i + 1) % peers) for i in range(peers)]
        down = [(j, i) for i, j in up]
        last = lax.slice_in_dim(shard, length - width, length, axis=dim)
        leading = lax.slice_in_dim(shard, 0, width, axis=dim)
        before = lax.ppermute(last, axis, up)
        after = lax.ppermute(leading, axis, down)
        shard = jnp.concatenate([before, shard, after], axis=dim)
    return shard


def shifted(block, axis, distance):
    devices = range(lax.axis_size(axis))
    route = [((i - distance) % len(devices), i) for i in devices]
    return lax.ppermute(block, axis, route)


def stencil_table(anchor, weights, length, offset, periodic):
    count = anchor.shape[0]
    cell_index = lax.broadcasted_iota(jnp.int32, (4, length, count), 1)
    tap_index = lax.broadcasted_iota(jnp.int32, (4, length, count), 0)
    target = anchor[None, None, :] + tap_index + offset
    if periodic:
        target = target % length
    chosen = jnp.where(target == cell_index, weights[:, None, :], jnp.zeros((), weights.dtype))
    return jnp.sum(chosen, axis=0)


def spread_cells(charge, anchor, weights, extent_x, extent_y, offset, length):
    table_x = stencil_table(anchor[0], weights[0] * charge[None, :], extent_x, offset, False)
    table_y = stencil_table(anchor[1], weights[1], extent_y, offset, False)
    table_z = stencil_table(anchor[2], weights[2], length, 0, True)
    planes = (table_x[:, None, :] * table_y[None, :, :]).reshape(extent_x * extent_y, -1)
    return jnp.dot(planes, table_z.T, precision=highest).reshape(extent_x, extent_y, length)


def interpolate(padded, anchor, weights, slopes):
    extent_x, extent_y, length = padded.shape
    table_x = stencil_table(anchor[0], weights[0], extent_x, 2, False)
    slope_x = stencil_table(anchor[0], slopes[0], extent_x, 2, False)
    table_y = stencil_table(anchor[1], weights[1], extent_y, 2, False)
    slope_y = stencil_table(anchor[1], slopes[1], extent_y, 2, False)
    table_z = stencil_table(anchor[2], weights[2], length, 0, True)
    slope_z = stencil_table(anchor[2], slopes[2], length, 0, True)
    flat = padded.reshape(extent_x * extent_y, length)
    along = jnp.dot(flat, table_z, precision=highest).reshape(extent_x, extent_y, -1)
    slant = jnp.dot(flat, slope_z, precision=highest).reshape(extent_x, extent_y, -1)
    over_y = jnp.sum(along * table_y[None], axis=1)
    value = jnp.sum(table_x * over_y, axis=0)
    field_x = -jnp.sum(slope_x * over_y, axis=0)
    over_x = jnp.sum(along * table_x[:, None, :], axis=0)
    field_y = -jnp.sum(slope_y * over_x, axis=0)
    slant_y = jnp.sum(slant * table_y[None], axis=1)
    field_z = -jnp.sum(table_x * slant_y, axis=0)
    return (value, jnp.stack([field_x, field_y, field_z]))


def fitted_charge(
    nearby,
    listed,
    count,
    embed_scale,
    embed_bias,
    desc_gain,
    fit_in,
    fit_bias,
    fit_hidden,
    fit_bias_two,
    fit_out,
):
    atoms = listed.shape[1]
    center = nearby[:, 4 * atoms : 5 * atoms]
    picked = jnp.take(nearby, listed.reshape(-1), axis=1).reshape(3, listed.shape[0], atoms)
    delta = picked - center[:, None, :]
    radius = jnp.sqrt(jnp.sum(delta * delta, axis=0))
    smooth = 1.0 / (1.0 + radius / radius_scale)
    factor = smooth / (radius + radius_scale)
    envelope = jnp.concatenate([smooth[None], delta * factor[None]], axis=0)
    embed = jnp.tanh(smooth[None] * embed_scale[:, None, None] + embed_bias[:, None, None])
    mixed = jnp.einsum("ekn,ckn->ecn", embed, envelope, precision=highest)
    descriptor = jnp.einsum("ecn,acn->ean", mixed, mixed[:AXIS], precision=highest).reshape(
        -1, atoms
    )
    scaling = lax.rsqrt(jnp.mean(descriptor * descriptor, axis=0) + norm_floor)
    normed = (descriptor * scaling[None, :] * desc_gain[:, None]).astype(jnp.bfloat16)
    first = jnp.tanh(
        jnp.dot(fit_in, normed, preferred_element_type=jnp.float32) + fit_bias[:, None]
    )
    second = (
        jnp.tanh(
            jnp.dot(fit_hidden, first.astype(jnp.bfloat16), preferred_element_type=jnp.float32)
            + fit_bias_two[:, None]
        )
        + first
    )
    charge = jnp.sum(fit_out[:, None] * second, axis=0)
    slot_index = lax.broadcasted_iota(jnp.int32, (atoms,), 0)
    return jnp.where(slot_index < count, charge, jnp.zeros((), charge.dtype))


def wave_number(index, length):
    signed = jnp.where(index > length // 2, index - length, index)
    return signed.astype(jnp.float32) * (full_turn / length)


def green_values(index_x, index_y, index_z, length):
    wave_x = wave_number(index_x, length)
    wave_y = wave_number(index_y, length)
    wave_z = wave_number(index_z, length)
    square = wave_x * wave_x + wave_y * wave_y + wave_z * wave_z
    safe = jnp.where(square > 0, square, 1.0)
    value = 2.0 * full_turn * jnp.exp(-0.5 * screen_width * screen_width * square) / safe
    keep = (square > 0) & (index_z != length // 2)
    return jnp.where(keep, value, 0.0)


def wave_tables(length, count):
    rows = lax.broadcasted_iota(jnp.int32, (length, count), 0)
    cols = lax.broadcasted_iota(jnp.int32, (length, count), 1)
    angle = (rows * cols % length).astype(jnp.float32) * (full_turn / length)
    return (jnp.cos(angle), jnp.sin(angle))


def along_axis(real_part, imag_part, cosine, sine, sign, form):
    real_cos = jnp.einsum(form, real_part, cosine, precision=highest)
    real_sin = jnp.einsum(form, real_part, sine, precision=highest)
    imag_cos = jnp.einsum(form, imag_part, cosine, precision=highest)
    imag_sin = jnp.einsum(form, imag_part, sine, precision=highest)
    return (real_cos + sign * imag_sin, imag_cos - sign * real_sin)


def local_mesh(
    positions,
    neighbours,
    live_count,
    stencil_base,
    spline_weight,
    spline_slope,
    embed_scale,
    embed_bias,
    desc_gain,
    fit_in,
    fit_bias,
    fit_hidden,
    fit_bias_two,
    fit_out,
):
    columns_y = lax.axis_size("gy")
    width_x = GRID // lax.axis_size("gx")
    width_y = GRID // columns_y
    atoms = positions.shape[3]
    beside_all = padded_2(positions, (("gx", 1), ("gy", 2)), 1)
    block_x = lax.broadcasted_iota(jnp.int32, (3, 3, atoms), 0) - 1
    block_y = lax.broadcasted_iota(jnp.int32, (3, 3, atoms), 1) - 1
    offsets = jnp.stack([block_x * width_x, block_y * width_y, jnp.zeros_like(block_x)]).astype(
        jnp.float32
    )
    nearby = (beside_all + offsets).reshape(3, 9 * atoms)
    charge = fitted_charge(
        nearby,
        neighbours[:, 0, 0, :],
        live_count[0, 0],
        embed_scale,
        embed_bias,
        desc_gain,
        fit_in,
        fit_bias,
        fit_hidden,
        fit_bias_two,
        fit_out,
    )
    anchor = stencil_base[:, 0, 0, :]
    weights = spline_weight[:, :, 0, 0, :]
    slopes = spline_slope[:, :, 0, 0, :]
    spread = spread_cells(charge, anchor, weights, width_x + 4, width_y + 4, 2, GRID)
    inner = spread[2 : width_x + 2]
    for stride in (1, -1):
        piece = spread[width_x + 2 :] if stride == 1 else spread[:2]
        moved = shifted(piece, "gx", stride)
        if stride == 1:
            inner = inner.at[:2].add(moved)
        else:
            inner = inner.at[width_x - 2 :].add(moved)
    density = inner[:, 2 : width_y + 2]
    for stride in (1, -1):
        piece = inner[:, width_y + 2 :] if stride == 1 else inner[:, :2]
        moved = shifted(piece, "gy", stride)
        if stride == 1:
            density = density.at[:, :2].add(moved)
        else:
            density = density.at[:, width_y - 2 :].add(moved)
    freqs = GRID // 2
    fold_weight = jnp.where(jnp.arange(freqs) == 0, 1.0, 2.0).astype(jnp.float32) / GRID
    cosine_z, sine_z = wave_tables(GRID, freqs)
    flat = density.reshape(width_x * width_y, GRID)
    real_part = jnp.dot(flat, cosine_z, precision=highest).reshape(width_x, width_y, freqs)
    imag_part = -jnp.dot(flat, sine_z, precision=highest).reshape(width_x, width_y, freqs)
    real_part, imag_part = (
        lax.all_to_all(real_part, "gy", split_axis=2, concat_axis=1, tiled=True),
        lax.all_to_all(imag_part, "gy", split_axis=2, concat_axis=1, tiled=True),
    )
    cosine, sine = wave_tables(GRID, GRID)
    real_part, imag_part = along_axis(real_part, imag_part, cosine, sine, 1.0, "xym,yk->xkm")
    real_part, imag_part = (
        lax.all_to_all(real_part, "gx", split_axis=1, concat_axis=0, tiled=True),
        lax.all_to_all(imag_part, "gx", split_axis=1, concat_axis=0, tiled=True),
    )
    real_part, imag_part = along_axis(real_part, imag_part, cosine, sine, 1.0, "xym,xk->kym")
    span_y = real_part.shape[1]
    span_z = real_part.shape[2]
    index_x = lax.broadcasted_iota(jnp.int32, (GRID, span_y, span_z), 0)
    index_y = lax.axis_index("gx") * span_y + lax.broadcasted_iota(
        jnp.int32, (GRID, span_y, span_z), 1
    )
    index_z = lax.axis_index("gy") * span_z + lax.broadcasted_iota(
        jnp.int32, (GRID, span_y, span_z), 2
    )
    green = green_values(index_x, index_y, index_z, GRID)
    real_part = real_part * green
    imag_part = imag_part * green
    back_cos = cosine / GRID
    back_sin = sine / GRID
    real_part, imag_part = along_axis(real_part, imag_part, back_cos, back_sin, -1.0, "xym,xk->kym")
    real_part, imag_part = (
        lax.all_to_all(real_part, "gx", split_axis=0, concat_axis=1, tiled=True),
        lax.all_to_all(imag_part, "gx", split_axis=0, concat_axis=1, tiled=True),
    )
    real_part, imag_part = along_axis(real_part, imag_part, back_cos, back_sin, -1.0, "xym,yk->xkm")
    real_part, imag_part = (
        lax.all_to_all(real_part, "gy", split_axis=1, concat_axis=2, tiled=True),
        lax.all_to_all(imag_part, "gy", split_axis=1, concat_axis=2, tiled=True),
    )
    rows_y = real_part.shape[1]
    flat_real = real_part.reshape(width_x * rows_y, freqs)
    flat_imag = imag_part.reshape(width_x * rows_y, freqs)
    summed_cos = (cosine_z * fold_weight[None, :]).T
    summed_sin = (sine_z * fold_weight[None, :]).T
    potential = jnp.dot(flat_real, summed_cos, precision=highest) - jnp.dot(
        flat_imag, summed_sin, precision=highest
    )
    potential = potential.reshape(width_x, rows_y, GRID)
    padded = padded_2(potential, (("gx", 0), ("gy", 1)), 2)
    value, field = interpolate(padded, anchor, weights, slopes)
    energy = (0.5 * charge * value).reshape(1, 1, atoms)
    force = (charge[None, :] * field).reshape(3, 1, 1, atoms)
    return (energy, force)


def solution(mesh):
    def local(positions, *rest):
        columns_x, columns_y = (lax.axis_size("gx"), lax.axis_size("gy"))
        sites = columns_x * columns_y * positions.shape[3]
        whole = GRID % (16 * columns_x) == 0 and GRID % (16 * columns_y) == 0
        few = whole and sites <= 8 * GRID * 2
        return (local_sites if few and positions.shape[3] == LANES else local_mesh)(positions, *rest)

    placed = (
        P(None, "gx", "gy", None),
        P(None, "gx", "gy", None),
        P("gx", "gy"),
        P(None, "gx", "gy", None),
        P(None, None, "gx", "gy", None),
        P(None, None, "gx", "gy", None),
        P(),
        P(),
        P(),
        P(),
        P(),
        P(),
        P(),
        P(),
    )
    return jax.shard_map(
        local,
        mesh=mesh,
        in_specs=placed,
        out_specs=(P("gx", "gy", None), P(None, "gx", "gy", None)),
        check_vma=False,
    )
```
